128 devices in a mesh: lat: 32 (over z, y, x_hi), lev: 4 (over x_lo, core).
Axes of the slice: x: 4 (x_hi: 2, x_lo: 2; x = x_hi * 2 + x_lo), y: 4, z: 4, core: 2. Of those that a mesh axis runs over, the one named last changes fastest.
Arguments:
- spec_in: bfloat16 [192, 171, 4, 512], P('lat', None, None, 'lev'), may hold values from -6 to 6
- cotangent: bfloat16 [192, 171, 4, 512], P('lat', None, None, 'lev'), may hold values from -6 to 6
- legendre: bfloat16 [192, 171, 256], P('lat'), may hold values from -0.4375 to 0.4375
- quad_weights: float32 [256], replicated, may hold values from 0.5 to 2
- wave_order: int32 [192], replicated, may hold values from 0 to 191, each once
- norm_gain: float32 [256], replicated, may hold values from 0.5 to 1.5
- weight_in: bfloat16 [256, 512], replicated, may hold values from -0.375 to 0.375
- bias_in: float32 [512], replicated, may hold values from -3 to 3
- weight_mid: bfloat16 [512, 512], replicated, may hold values from -0.25 to 0.25
- bias_mid: float32 [512], replicated, may hold values from -3 to 3
- weight_out: bfloat16 [512, 256], replicated, may hold values from -0.25 to 0.25
Outputs:
- grad_spec: float32 [192, 171, 4, 512], P('lat', None, None, 'lev')
- grad_gain: float32 [256], replicated
- grad_w_in: float32 [256, 512], replicated
- grad_b_in: float32 [512], replicated
- grad_w_mid: float32 [512, 512], replicated
- grad_b_mid: float32 [512], replicated
- grad_w_out: float32 [512, 256], replicated
The draws below stay inside these ranges and needn't reach their ends.
Inputs may be any that keep to these rules, and one draw needn't show every extreme that they name: `wave_order`: each of 0 to 191 appears once; a slot holding 171 or more is unused.
All inputs are finite; a program needn't handle non-finite values.
Results may differ from the reference program's by a relative error of at most 0.007.
Values may be sent and summed in bfloat16 or wider, within the bound.
A program may use at most 128 MiB of HBM per device.

```python
import math
import jax
import jax.numpy as jnp
from jax import lax

WAVES = 171
SLOTS = 192
NLAT = 256
NLON = 512
HIDDEN_SIZE = 512
MEMBERS = 4
CHANNELS = 256
COLUMNS = 524288


def levels(stream_key, extent, cuts, least, high):
    level = 1.0
    for axis_at, shards_of in cuts:
        steps = jax.random.uniform(jax.random.fold_in(jax.random.fold_in(stream_key, 6), axis_at), (shards_of,), jnp.float32, least / len(cuts), high / len(cuts))
        level = level * jnp.repeat(jnp.exp(steps), extent[axis_at] // shards_of).reshape((-1,) + (1,) * (len(extent) - 1 - axis_at))
    return level


def noise(own_key, shape, spread, limit, split=(), kind=jnp.bfloat16):
    loudness = levels(own_key, shape, split, -0.22, 0.18) if split else 1.0
    drawn = jax.random.normal(own_key, shape, jnp.float32) * spread * loudness
    return jnp.minimum(jnp.maximum(drawn, -limit), limit).astype(kind)


def setup_inputs(seed: int = 0) -> dict:
    key_of = jax.random.split(jax.random.key(seed), 12)
    return {
        "spec_in": noise(key_of[0], (SLOTS, WAVES, MEMBERS, 2 * CHANNELS), 1.0, 6.0, ((0, 32), (3, 4))),
        "cotangent": noise(key_of[1], (SLOTS, WAVES, MEMBERS, 2 * CHANNELS), 1.0, 6.0, ((0, 32), (3, 4))),
        "legendre": noise(key_of[2], (SLOTS, WAVES, NLAT), WAVES ** -0.5, 0.4375, ((0, 32),)),
        "quad_weights": jnp.clip(jnp.exp(jax.random.uniform(key_of[3], (NLAT,), jnp.float32, math.log(0.5), math.log(2.0))), 0.5, 2.0),
        "wave_order": jax.random.permutation(key_of[4], SLOTS).astype(jnp.int32),
        "norm_gain": jnp.clip(1.0 + 0.1 * jax.random.normal(key_of[5], (CHANNELS,), jnp.float32), 0.5, 1.5),
        "weight_in": noise(key_of[6], (CHANNELS, HIDDEN_SIZE), CHANNELS ** -0.5, 0.375),
        "bias_in": noise(key_of[7], (HIDDEN_SIZE,), 0.5, 3.0, (), jnp.float32),
        "weight_mid": noise(key_of[8], (HIDDEN_SIZE, HIDDEN_SIZE), HIDDEN_SIZE ** -0.5, 0.25),
        "bias_mid": noise(key_of[9], (HIDDEN_SIZE,), 0.5, 3.0, (), jnp.float32),
        "weight_out": noise(key_of[10], (HIDDEN_SIZE, CHANNELS), HIDDEN_SIZE ** -0.5, 0.25),
    }


time_step = 0.5
norm_eps = 1e-06

def spectral_masks(waves_held, degree_count):
    degree = jnp.arange(degree_count, dtype=jnp.int32)
    living = (waves_held[:, None] <= degree[None, :]) & (waves_held[:, None] < WAVES)
    ratio = (degree * (degree + 1)).astype(jnp.float32) / float(WAVES * (WAVES - 1))
    factor = (1.0 / (1.0 + ratio * ratio)).astype(jnp.float32)
    shrink = jnp.where(living, factor[None, :], jnp.zeros_like(factor)[None, :])
    return (living, shrink)

def fourier_table(waves_all):
    longitude = jnp.arange(NLON, dtype=jnp.int32)
    phase_steps = waves_all[:, None] * longitude[None, :] % NLON
    angles = phase_steps.astype(jnp.float32) * (2.0 * math.pi / NLON)
    weight_scale = jnp.where(waves_all < WAVES, math.sqrt(2.0 / NLON), 0.0).astype(jnp.float32)[:, None]
    return jnp.stack([jnp.cos(angles) * weight_scale, -jnp.sin(angles) * weight_scale], axis=1).astype(jnp.bfloat16)

def contract_rows(left, right):
    return lax.dot_general(left, right, (((0,), (0,)), ((), ())), preferred_element_type=jnp.float32)

def contract_cols(left, right):
    return lax.dot_general(left, right, (((1,), (1,)), ((), ())), preferred_element_type=jnp.float32)

def column_grads(columns, column_cot, norm_gain, weight_in, bias_in, weight_mid, bias_mid, weight_out):
    inputs = columns.astype(jnp.float32)
    inverse = lax.rsqrt(lax.optimization_barrier(jnp.mean(inputs * inputs, axis=1, keepdims=True)) + norm_eps)
    gains = norm_gain.astype(jnp.float32)
    normed = (inputs * inverse * gains).astype(jnp.bfloat16)
    pre_one = jnp.dot(normed, weight_in, preferred_element_type=jnp.float32) + bias_in
    sig_one = jax.nn.sigmoid(pre_one)
    act_one = (pre_one * sig_one).astype(jnp.bfloat16)
    pre_two = jnp.dot(act_one, weight_mid, preferred_element_type=jnp.float32) + bias_mid
    sig_two = jax.nn.sigmoid(pre_two)
    act_two = (pre_two * sig_two).astype(jnp.bfloat16)
    gradient_third = contract_rows(act_two, column_cot)
    back_two = contract_cols(column_cot, weight_out)
    delta_two = (back_two * sig_two * (1.0 + pre_two * (1.0 - sig_two))).astype(jnp.bfloat16)
    gradient_second = contract_rows(act_one, delta_two)
    offset_second = lax.optimization_barrier(jnp.sum(delta_two.astype(jnp.float32), axis=0))
    back_one = contract_cols(delta_two, weight_mid)
    delta_one = (back_one * sig_one * (1.0 + pre_one * (1.0 - sig_one))).astype(jnp.bfloat16)
    gradient_first = contract_rows(normed, delta_one)
    offset_first = lax.optimization_barrier(jnp.sum(delta_one.astype(jnp.float32), axis=0))
    back_norm = contract_cols(delta_one, weight_in)
    gradient_gain = lax.optimization_barrier(jnp.sum(back_norm * inputs * inverse, axis=0))
    scaled = back_norm * gains
    grad_columns = inverse * scaled - inputs * inverse * inverse * inverse * lax.optimization_barrier(jnp.mean(scaled * inputs, axis=1, keepdims=True))
    return (grad_columns.astype(jnp.bfloat16), (gradient_gain, gradient_first, offset_first, gradient_second, offset_second, gradient_third))

def unpack_parts(packed):
    return jnp.transpose(packed.reshape(SLOTS, WAVES, MEMBERS, CHANNELS, 2), (0, 1, 2, 4, 3))

def reference(spec_in, cotangent, legendre, quad_weights, wave_order, norm_gain, weight_in, bias_in, weight_mid, bias_mid, weight_out):
    highest = lax.Precision.HIGHEST
    spec_in = unpack_parts(spec_in)
    cotangent = unpack_parts(cotangent)
    living, shrink = spectral_masks(wave_order, WAVES)
    basis_rows = jnp.where(living[:, :, None], legendre, jnp.zeros_like(legendre))
    wave_table = fourier_table(wave_order)
    basis_wide = basis_rows.astype(jnp.float32)
    table_wide = wave_table.astype(jnp.float32)
    fourier = jnp.einsum('slt,slepc->stepc', basis_wide, spec_in.astype(jnp.float32), precision=highest).astype(jnp.bfloat16)
    pushed = (time_step * cotangent.astype(jnp.float32) * shrink[:, :, None, None, None]).astype(jnp.bfloat16)
    pulled = jnp.einsum('slt,slepc->stepc', basis_wide, pushed.astype(jnp.float32), precision=highest)
    pulled = (quad_weights[None, :, None, None, None] * pulled).astype(jnp.bfloat16)
    grid_values = jnp.einsum('spo,stepc->otec', table_wide, fourier.astype(jnp.float32), precision=highest).astype(jnp.bfloat16)
    grid_cot = jnp.einsum('spo,stepc->otec', table_wide, pulled.astype(jnp.float32), precision=highest).astype(jnp.bfloat16)
    member_rows = jnp.transpose(grid_values, (2, 0, 1, 3)).reshape(MEMBERS, NLON * NLAT, CHANNELS)
    member_cots = jnp.transpose(grid_cot, (2, 0, 1, 3)).reshape(MEMBERS, NLON * NLAT, CHANNELS)

    def per_member(pair):
        return column_grads(pair[0], pair[1], norm_gain, weight_in, bias_in, weight_mid, bias_mid, weight_out)
    grad_rows, grads_all = lax.map(per_member, (member_rows, member_cots))
    factor = float(COLUMNS) ** (-0.5)
    grads = tuple((lax.optimization_barrier(jnp.sum(piece, axis=0)) * factor for piece in grads_all))
    grad_grid = jnp.transpose(grad_rows.reshape(MEMBERS, NLON, NLAT, CHANNELS), (1, 2, 0, 3))
    back_fourier = jnp.einsum('spo,otec->stepc', table_wide, grad_grid.astype(jnp.float32), precision=highest).astype(jnp.bfloat16)
    grad_spec = cotangent.astype(jnp.float32) * shrink[:, :, None, None, None] + jnp.einsum('slt,stepc->slepc', basis_wide, back_fourier.astype(jnp.float32), precision=highest)
    grad_spec = jnp.transpose(grad_spec, (0, 1, 2, 4, 3)).reshape(SLOTS, WAVES, MEMBERS, 2 * CHANNELS)
    return (grad_spec, grads[0], grads[1], grads[2], grads[3], grads[4], grads[5])
```

```python
import functools
import math

import jax
import jax.numpy as jnp
import numpy as np
from jax import lax
from jax.experimental import pallas as pl
from jax.experimental.pallas import tpu as pltpu
from jax.sharding import PartitionSpec as P

WAVES = 171
NLAT = 256
NLON = 512
MEMBERS = 4

time_step = 0.5
norm_eps = 1e-06
MESH = pl.DeviceIdType.MESH


def spectral_masks(waves_held, degree_count):
    degree = jnp.arange(degree_count, dtype=jnp.int32)
    living = (waves_held[:, None] <= degree[None, :]) & (waves_held[:, None] < WAVES)
    ratio = (degree * (degree + 1)).astype(jnp.float32) / float(WAVES * (WAVES - 1))
    factor = 1.0 / (1.0 + ratio * ratio)
    shrink = jnp.where(living, factor[None, :], jnp.zeros_like(factor)[None, :])
    return (living, shrink)


def fourier_tables(waves_all):
    longitude = jnp.arange(NLON, dtype=jnp.int32)
    phase_steps = waves_all[:, None] * longitude[None, :] % NLON
    angles = phase_steps.astype(jnp.float32) * (2.0 * math.pi / NLON)
    weight_scale = jnp.where(waves_all < WAVES, math.sqrt(2.0 / NLON), 0.0).astype(jnp.float32)[
        :, None
    ]
    table = jnp.concatenate(
        [jnp.cos(angles) * weight_scale, -jnp.sin(angles) * weight_scale], axis=0
    ).astype(jnp.bfloat16)
    return table


def exchange(n_lat, n_lev, forward, src_ref, dst_ref, send_sem, recv_sem, own_sem):
    n = n_lat * n_lev
    i = lax.axis_index("lat")
    j = lax.axis_index("lev")
    me = i * n_lev + j
    pairs = 3

    def ends(peer_i, peer_j, peer):
        if forward:
            return src_ref.at[peer], dst_ref.at[:, :, :, j, pl.ds(i * pairs, pairs)]
        return src_ref.at[:, :, peer_j, pl.ds(peer_i * pairs, pairs)], dst_ref.at[me]

    def start(step, carry):
        peer = lax.rem(me + step, n)
        peer_i = peer // n_lev
        peer_j = lax.rem(peer, n_lev)
        src, dst = ends(peer_i, peer_j, peer)
        pltpu.make_async_remote_copy(
            src_ref=src, dst_ref=dst, send_sem=send_sem, recv_sem=recv_sem,
            device_id=(peer_i, peer_j), device_id_type=MESH,
        ).start()
        return carry

    src, dst = ends(i, j, me)
    own = pltpu.make_async_copy(src, dst, own_sem)
    own.start()
    lax.fori_loop(1, n, start, 0)
    own.wait()
    many = (src_ref if forward else dst_ref).at[pl.ds(0, n - 1)]
    pltpu.make_async_copy(many, many, send_sem).wait()
    pltpu.make_async_copy(many, many, recv_sem).wait()


def exchange_call(array, out_shape, n_lat, n_lev, forward):
    return pl.pallas_call(
        functools.partial(exchange, n_lat, n_lev, forward),
        out_shape=jax.ShapeDtypeStruct(out_shape, array.dtype),
        in_specs=[pl.BlockSpec(memory_space=pl.ANY)],
        out_specs=pl.BlockSpec(memory_space=pl.ANY),
        scratch_shapes=[pltpu.SemaphoreType.DMA] * 3,
        compiler_params=pltpu.CompilerParams(has_side_effects=True),
        name="exchange_out" if forward else "exchange_back",
    )(array)


def dot(a, b, dims):
    return lax.dot_general(a, b, (dims, ((), ())), preferred_element_type=jnp.float32)


def sigmoid(z):
    return 0.5 * jnp.tanh(0.5 * z) + 0.5


def join_levels(parts):
    half = parts[0].shape[1] // 2
    rows = []
    for p in range(2):
        rows.append(
            jnp.concatenate([a[:, p * half : (p + 1) * half] for a in parts], axis=1)
        )
    return jnp.concatenate(rows, axis=0)


def column_kernel(
    recv_ref, table_ref, table_t_ref, gain_ref, w_in_ref, b_in_ref, w_mid_ref, b_mid_ref,
    w_out_ref, back_ref, g_gain_ref, g_in_ref, g_b_in_ref, g_mid_ref, g_b_mid_ref, g_out_ref,
):
    first = pl.program_id(0) == 0

    @pl.when(first)
    def _():
        for ref in (g_gain_ref, g_in_ref, g_b_in_ref, g_mid_ref, g_b_mid_ref, g_out_ref):
            ref[...] = jnp.zeros_like(ref)

    levels = recv_ref.shape[3]
    state = join_levels([recv_ref[0, 0, 0, j] for j in range(levels)])
    cot = join_levels([recv_ref[1, 0, 0, j] for j in range(levels)])
    nn, nt, tn = (((1,), (0,)), ((1,), (1,)), ((0,), (0,)))
    columns = dot(table_t_ref[...], state, nn).astype(jnp.bfloat16)
    column_cot = dot(table_t_ref[...], cot, nn).astype(jnp.bfloat16)
    gain = gain_ref[...]
    inputs = columns.astype(jnp.float32)
    inverse = lax.rsqrt(jnp.mean(inputs * inputs, axis=1, keepdims=True) + norm_eps)
    normed = (inputs * inverse * gain).astype(jnp.bfloat16)
    pre_one = dot(normed, w_in_ref[...], nn) + b_in_ref[...]
    sig_one = sigmoid(pre_one)
    act_one = (pre_one * sig_one).astype(jnp.bfloat16)
    slope_one = sig_one * (1.0 + pre_one * (1.0 - sig_one))
    pre_two = dot(act_one, w_mid_ref[...], nn) + b_mid_ref[...]
    sig_two = sigmoid(pre_two)
    act_two = (pre_two * sig_two).astype(jnp.bfloat16)
    slope_two = sig_two * (1.0 + pre_two * (1.0 - sig_two))
    back_two = dot(column_cot, w_out_ref[...], nt)
    delta_two32 = back_two * slope_two
    delta_two = delta_two32.astype(jnp.bfloat16)
    back_one = dot(delta_two, w_mid_ref[...], nt)
    delta_one = (back_one * slope_one).astype(jnp.bfloat16)
    back_norm = dot(delta_one, w_in_ref[...], nt)
    scaled = back_norm * gain
    grad_columns = inverse * scaled - inputs * (inverse * inverse * inverse) * jnp.mean(
        scaled * inputs, axis=1, keepdims=True
    )
    grad_columns = grad_columns.astype(jnp.bfloat16)
    back = dot(table_ref[...], grad_columns, nn).astype(jnp.bfloat16)
    slots = back.shape[0] // 2
    half = back.shape[1] // levels
    for j in range(levels):
        back_ref[0, 0, j] = jnp.concatenate(
            [
                back[p * slots : (p + 1) * slots, j * half : (j + 1) * half]
                for p in range(2)
            ],
            axis=1,
        )
    g_out_ref[...] += dot(act_two, column_cot, tn)
    g_mid_ref[...] += dot(act_one, delta_two, tn)
    g_in_ref[...] += dot(normed, delta_one, tn)
    g_b_mid_ref[...] += jnp.sum(delta_two.astype(jnp.float32), axis=0, keepdims=True)
    g_b_in_ref[...] += jnp.sum(delta_one.astype(jnp.float32), axis=0, keepdims=True)
    g_gain_ref[...] += jnp.sum(back_norm * inputs * inverse, axis=0, keepdims=True)


def column_call(recv, table, gain, w_in, b_in, w_mid, b_mid, w_out):
    kinds, rows, members, levels, slots, lanes = recv.shape
    table_t = table.T
    params = (table, table_t, gain[None], w_in, b_in[None], w_mid, b_mid[None], w_out)
    whole = lambda a: pl.BlockSpec(a.shape, lambda b: (0,) * a.ndim)
    f32 = jnp.float32
    grads = [
        jax.ShapeDtypeStruct(s, f32)
        for s in (
            (1, gain.shape[0]), w_in.shape, (1, b_in.shape[0]), w_mid.shape, (1, b_mid.shape[0]),
            w_out.shape,
        )
    ]
    back = jax.ShapeDtypeStruct((rows, members, levels, slots, lanes), recv.dtype)
    return pl.pallas_call(
        column_kernel,
        grid=(rows * members,),
        out_shape=[back] + grads,
        in_specs=[
            pl.BlockSpec(
                (kinds, 1, 1, levels, slots, lanes),
                lambda b: (0, b // members, b % members, 0, 0, 0),
            )
        ]
        + [whole(a) for a in params],
        out_specs=[
            pl.BlockSpec(
                (1, 1, levels, slots, lanes), lambda b: (b // members, b % members, 0, 0, 0)
            )
        ]
        + [whole(a) for a in grads],
        compiler_params=pltpu.CompilerParams(
            dimension_semantics=("arbitrary",), vmem_limit_bytes=56 * 1024 * 1024
        ),
        name="columns",
    )(recv, *params)


def local(
    n_lat, n_lev, spec_in, cotangent, legendre, quad_weights, wave_order, norm_gain, weight_in,
    bias_in, weight_mid, bias_mid, weight_out,
):
    bf16 = jnp.bfloat16
    n = n_lat * n_lev
    slots_here, degrees, members, lanes = spec_in.shape
    rows = NLAT // n
    own_waves = lax.dynamic_slice_in_dim(wave_order, lax.axis_index("lat") * slots_here, slots_here)
    living, shrink = spectral_masks(own_waves, degrees)
    basis_rows = jnp.where(living[:, :, None], legendre, jnp.zeros_like(legendre))
    table = fourier_tables(wave_order)
    lane = np.arange(lanes)
    apart = np.zeros((lanes, lanes), np.float32)
    apart[lane, (lane % 2) * (lanes // 2) + lane // 2] = 1.0
    apart = jnp.asarray(apart, bf16)

    state = jnp.einsum("slek,kq->sleq", spec_in, apart, preferred_element_type=jnp.float32)
    pushed = (time_step * cotangent.astype(jnp.float32) * shrink[:, :, None, None]).astype(bf16)
    pushed = jnp.einsum("slek,kq->sleq", pushed, apart, preferred_element_type=jnp.float32)
    fourier = jnp.einsum(
        "slt,sleq->steq", basis_rows, state.astype(bf16), preferred_element_type=jnp.float32
    ).astype(bf16)
    pulled = jnp.einsum(
        "slt,sleq->steq", basis_rows, pushed.astype(bf16), preferred_element_type=jnp.float32
    )
    pulled = (quad_weights[None, :, None, None] * pulled).astype(bf16)
    both = jnp.stack([fourier, pulled])
    both = both.reshape(2, slots_here, n, rows, members, lanes).transpose(2, 0, 3, 4, 1, 5)
    both = both.reshape(n, 2, rows, members, slots_here // 2, 2, lanes)
    recv = exchange_call(
        both, (2, rows, members, n_lev, n_lat * slots_here // 2, 2, lanes), n_lat, n_lev, True
    )
    recv = recv.reshape(2, rows, members, n_lev, n_lat * slots_here, lanes)
    back, *grads = column_call(
        recv, table, norm_gain, weight_in, bias_in, weight_mid, bias_mid, weight_out
    )
    back = back.reshape(rows, members, n_lev, n_lat * slots_here // 2, 2, lanes)
    summed = lax.psum(tuple(grads), ("lat", "lev"))
    landed = exchange_call(
        back, (n, rows, members, slots_here // 2, 2, lanes), n_lat, n_lev, False
    )
    landed = landed.reshape(n * rows, members, slots_here, lanes)
    landed = jnp.einsum(
        "tesq,kq->stek", landed, apart, preferred_element_type=jnp.float32
    ).astype(bf16)
    grad_spec = cotangent.astype(jnp.float32) * shrink[:, :, None, None] + jnp.einsum(
        "slt,stek->slek", basis_rows, landed, preferred_element_type=jnp.float32
    )
    factor = float(MEMBERS * NLAT * NLON) ** (-0.5)
    out = [piece * factor for piece in summed]
    return (grad_spec, out[0][0], out[1], out[2][0], out[3], out[4][0], out[5])


def solution(mesh):
    split = P("lat", None, None, "lev")
    placed = (split, split, P("lat", None, None)) + (P(),) * 8
    return jax.shard_map(
        functools.partial(local, mesh.shape["lat"], mesh.shape["lev"]),
        mesh=mesh,
        in_specs=placed,
        out_specs=(split,) + (P(),) * 6,
        check_vma=False,
    )
```

```python
import functools
import math

import jax
import jax.numpy as jnp
import numpy as np
from jax import lax
from jax.experimental import pallas as pl
from jax.experimental.pallas import tpu as pltpu
from jax.sharding import PartitionSpec as P

WAVES = 171
NLAT = 256
NLON = 512
MEMBERS = 4

time_step = 0.5
norm_eps = 1e-06
MESH = pl.DeviceIdType.MESH


def spectral_masks(waves_held, degree_count):
    degree = jnp.arange(degree_count, dtype=jnp.int32)
    living = (waves_held[:, None] <= degree[None, :]) & (waves_held[:, None] < WAVES)
    ratio = (degree * (degree + 1)).astype(jnp.float32) / float(WAVES * (WAVES - 1))
    factor = 1.0 / (1.0 + ratio * ratio)
    shrink = jnp.where(living, factor[None, :], jnp.zeros_like(factor)[None, :])
    return (living, shrink)


def fourier_tables(waves_all):
    longitude = jnp.arange(NLON, dtype=jnp.int32)
    phase_steps = waves_all[:, None] * longitude[None, :] % NLON
    angles = phase_steps.astype(jnp.float32) * (2.0 * math.pi / NLON)
    weight_scale = jnp.where(waves_all < WAVES, math.sqrt(2.0 / NLON), 0.0).astype(jnp.float32)[
        :, None
    ]
    table = jnp.concatenate(
        [jnp.cos(angles) * weight_scale, -jnp.sin(angles) * weight_scale], axis=0
    ).astype(jnp.bfloat16)
    return table


def part(value, size, of):
    return lax.rem(value // of, size)


def peer_at(step, i, j):
    away = lax.rem(step * 37, 128)
    z = lax.rem(i // 8 + lax.rem(away, 4), 4)
    y = lax.rem(part(i, 4, 2) + part(away, 4, 4), 4)
    x = lax.rem(lax.rem(i, 2) * 2 + j // 2 + part(away, 4, 16), 4)
    core = lax.rem(j + away // 64, 2)
    return z * 8 + y * 2 + x // 2, lax.rem(x, 2) * 2 + core


def chip_at(step, i, j):
    away = lax.rem(step * 37, 64)
    z = lax.rem(i // 8 + lax.rem(away, 4), 4)
    y = lax.rem(part(i, 4, 2) + part(away, 4, 4), 4)
    x = lax.rem(lax.rem(i, 2) * 2 + j // 2 + away // 16, 4)
    return z * 8 + y * 2 + x // 2, lax.rem(x, 2) * 2 + lax.rem(j, 2)


def send(src, dst, send_sem, recv_sem, peer):
    copy = pltpu.make_async_remote_copy(
        src_ref=src, dst_ref=dst, send_sem=send_sem, recv_sem=recv_sem,
        device_id=peer, device_id_type=MESH,
    )
    copy.start()
    return copy


def await_bytes(like, sem):
    pltpu.make_async_copy(like, like, sem).wait()


def exchange_out(n, src_ref, dst_ref, send_sem, recv_sem, own_sem):
    i, j = lax.axis_index("lat"), lax.axis_index("lev")
    slots, kinds = src_ref.shape[:2]

    def ends(kind, peer):
        return src_ref.at[:, kind, peer], dst_ref.at[kind, j, pl.ds(i * slots, slots)]

    def start(step, carry):
        peer = peer_at(step, i, j)
        for kind in range(kinds):
            send(*ends(kind, peer[0] * 4 + peer[1]), send_sem, recv_sem, peer)
        return carry

    for kind in range(kinds):
        pltpu.make_async_copy(*ends(kind, i * 4 + j), own_sem).start()
    lax.fori_loop(1, n, start, 0)
    await_bytes(src_ref.at[:, :, 0], own_sem)
    many = src_ref.at[:, :, pl.ds(0, n - 1)]
    await_bytes(many, send_sem)
    await_bytes(many, recv_sem)


def exchange_out_call(array, n_lat, n_lev):
    slots, kinds, n, two, lanes = array.shape
    return pl.pallas_call(
        functools.partial(exchange_out, n),
        out_shape=jax.ShapeDtypeStruct((kinds, n_lev, n_lat * slots, two, lanes), array.dtype),
        in_specs=[pl.BlockSpec(memory_space=pl.ANY)],
        out_specs=pl.BlockSpec(memory_space=pl.ANY),
        scratch_shapes=[pltpu.SemaphoreType.DMA] * 3,
        compiler_params=pltpu.CompilerParams(has_side_effects=True),
        name="exchange_out",
    )(array)


def exchange_back(
    n, back_ref, grads_ref, small_ref, landed_ref, total_ref, small_total_ref,
    own_half, their_half, rs_src, rs_recv, ag_src, small_recv, small_sum,
    pair_sems, back_sems, rs_sems, ag_sems, swap_sems, small_sems, small_back_sems, local_sems,
):
    i, j = lax.axis_index("lat"), lax.axis_index("lev")
    me = i * 4 + j
    core = lax.rem(j, 2)
    chip = i * 2 + j // 2
    chips = n // 2
    partner = (i, j + 1 - 2 * core)
    slots = landed_ref.shape[1]
    is_owner = me == 0

    pair = send(grads_ref.at[1 - core], their_half, pair_sems.at[0], pair_sems.at[1], partner)
    own = pltpu.make_async_copy(grads_ref.at[core], own_half, local_sems.at[0])
    own.start()
    stay = pltpu.make_async_copy(
        back_ref.at[:, j, pl.ds(i * slots, slots)], landed_ref.at[:, :, me], local_sems.at[1]
    )
    stay.start()

    @pl.when(jnp.logical_not(is_owner))
    def _():
        send(small_ref, small_recv.at[me], small_sems.at[0], small_sems.at[1], (0, 0))

    def start_back(step, carry):
        peer = peer_at(step, i, j)
        send(
            back_ref.at[:, peer[1], pl.ds(peer[0] * slots, slots)], landed_ref.at[:, :, me],
            back_sems.at[0], back_sems.at[1], peer,
        )
        return carry

    lax.fori_loop(1, n, start_back, 0)

    own.wait()
    pair.wait()
    rs_src[...] = (own_half[...] + their_half[...]).astype(rs_src.dtype).reshape(rs_src.shape)

    def start_rs(step, carry):
        peer = chip_at(step, i, j)
        send(
            rs_src.at[peer[0] * 2 + peer[1] // 2], rs_recv.at[chip],
            rs_sems.at[0], rs_sems.at[1], peer,
        )
        return carry

    lax.fori_loop(1, chips, start_rs, 0)

    @pl.when(is_owner)
    def _():
        mine = pltpu.make_async_copy(small_ref, small_recv.at[0], local_sems.at[2])
        mine.start()
        mine.wait()
        await_bytes(small_recv.at[pl.ds(0, n - 1)], small_sems.at[1])
        small_sum[...] = jnp.sum(small_recv[...], axis=0)

        def start_small(step, carry):
            peer = peer_at(step, i, j)
            send(
                small_sum, small_total_ref, small_back_sems.at[0], small_back_sems.at[1], peer
            )
            return carry

        lax.fori_loop(1, n, start_small, 0)
        mine = pltpu.make_async_copy(small_sum, small_total_ref, local_sems.at[2])
        mine.start()
        mine.wait()
        await_bytes(small_recv.at[pl.ds(0, n - 1)], small_back_sems.at[0])

    @pl.when(jnp.logical_not(is_owner))
    def _():
        await_bytes(small_ref, small_sems.at[0])

    rs_recv[chip] = rs_src[chip]
    await_bytes(rs_src.at[pl.ds(0, chips - 1)], rs_sems.at[1])
    ag_src[...] = jnp.sum(rs_recv[...].astype(jnp.float32), axis=0).astype(ag_src.dtype)

    def start_ag(step, carry):
        peer = chip_at(step, i, j)
        send(ag_src, total_ref.at[core, chip], ag_sems.at[0], ag_sems.at[1], peer)
        return carry

    lax.fori_loop(1, chips, start_ag, 0)
    mine = pltpu.make_async_copy(ag_src, total_ref.at[core, chip], local_sems.at[3])
    mine.start()
    mine.wait()
    await_bytes(rs_src.at[pl.ds(0, chips - 1)], rs_sems.at[0])
    await_bytes(rs_src.at[pl.ds(0, chips - 1)], ag_sems.at[1])
    swap = send(
        total_ref.at[core], total_ref.at[core], swap_sems.at[0], swap_sems.at[1], partner
    )
    await_bytes(rs_src.at[pl.ds(0, chips - 1)], ag_sems.at[0])
    stay.wait()
    many = landed_ref.at[:, :, pl.ds(0, n - 1)]
    await_bytes(many, back_sems.at[0])
    await_bytes(many, back_sems.at[1])

    @pl.when(jnp.logical_not(is_owner))
    def _():
        await_bytes(small_ref, small_back_sems.at[1])

    swap.wait()


def exchange_back_call(back, grads, small, n_lat, n_lev):
    members, _, all_slots, two, lanes = back.shape
    n = n_lat * n_lev
    bf16 = jnp.bfloat16
    grads = grads.reshape(2, -1, lanes)
    half = grads.shape[1]
    chips = n // 2
    slices = (chips, half // chips, lanes)
    return pl.pallas_call(
        functools.partial(exchange_back, n),
        out_shape=(
            jax.ShapeDtypeStruct((members, all_slots // n_lat, n, two, lanes), back.dtype),
            jax.ShapeDtypeStruct((2,) + slices, bf16),
            jax.ShapeDtypeStruct(small.shape, small.dtype),
        ),
        in_specs=[pl.BlockSpec(memory_space=pl.ANY)] * 3,
        out_specs=[pl.BlockSpec(memory_space=pl.ANY)] * 3,
        scratch_shapes=[
            pltpu.VMEM((half, lanes), jnp.float32),
            pltpu.VMEM((half, lanes), jnp.float32),
            pltpu.VMEM(slices, bf16),
            pltpu.VMEM(slices, bf16),
            pltpu.VMEM(slices[1:], bf16),
            pltpu.VMEM((n,) + small.shape, small.dtype),
            pltpu.VMEM(small.shape, small.dtype),
        ]
        + [pltpu.SemaphoreType.DMA((2,))] * 7
        + [pltpu.SemaphoreType.DMA((4,))],
        compiler_params=pltpu.CompilerParams(has_side_effects=True),
        name="exchange_back",
    )(back, grads, small)


def dot(a, b, dims):
    return lax.dot_general(a, b, (dims, ((), ())), preferred_element_type=jnp.float32)


def sigmoid(z):
    return 0.5 * jnp.tanh(0.5 * z) + 0.5


def join_levels(parts):
    half = parts[0].shape[1] // 2
    rows = []
    for p in range(2):
        rows.append(
            jnp.concatenate([a[:, p * half : (p + 1) * half] for a in parts], axis=1)
        )
    return jnp.concatenate(rows, axis=0)


def one_of_two(shape, long_dim, which):
    long = lax.broadcasted_iota(jnp.int32, shape, long_dim)
    short = lax.broadcasted_iota(jnp.int32, shape, 1 - long_dim)
    return jnp.where(long == 2 * short + which, 1.0, 0.0).astype(jnp.bfloat16)


NN, NT, TN = (((1,), (0,)), ((1,), (1,)), ((0,), (0,)))


def add_blocks(ref, start, value):
    rows, lanes = value.shape[0], ref.shape[1]
    for b in range(value.shape[1] // lanes):
        ref[pl.ds(start + b * rows, rows)] += value[:, b * lanes : (b + 1) * lanes]


def column_kernel(
    recv_ref, table_ref, table_t_ref, gain_ref, w_in_ref, b_in_ref, w_mid_ref, b_mid_ref,
    w_out_ref, back_ref, grads_ref, small_ref, syn_ref, ana_ref,
):
    waves, longitudes = table_ref.shape

    @pl.when(pl.program_id(0) == 0)
    def _():
        grads_ref[...] = jnp.zeros_like(grads_ref)
        small_ref[...] = jnp.zeros_like(small_ref)
        for r in range(2):
            span = pl.ds(r * longitudes, longitudes)
            syn_ref[span] = dot(
                table_t_ref[...], one_of_two((waves, 2 * waves), 1, r), NN
            ).astype(jnp.bfloat16)
            ana_ref[:, span] = dot(
                one_of_two((2 * waves, waves), 0, r), table_ref[...], NN
            ).astype(jnp.bfloat16)

    levels = recv_ref.shape[2]
    state = join_levels([recv_ref[0, 0, j] for j in range(levels)])
    cot = join_levels([recv_ref[1, 0, j] for j in range(levels)])
    columns = dot(syn_ref[...], state, NN).astype(jnp.bfloat16)
    column_cot = dot(syn_ref[...], cot, NN).astype(jnp.bfloat16)
    gain = gain_ref[...]
    inputs = columns.astype(jnp.float32)
    inverse = lax.rsqrt(jnp.mean(inputs * inputs, axis=1, keepdims=True) + norm_eps)
    normed = (inputs * inverse * gain).astype(jnp.bfloat16)
    pre_one = dot(normed, w_in_ref[...], NN) + b_in_ref[...]
    sig_one = sigmoid(pre_one)
    act_one = (pre_one * sig_one).astype(jnp.bfloat16)
    slope_one = sig_one * (1.0 + pre_one * (1.0 - sig_one))
    pre_two = dot(act_one, w_mid_ref[...], NN) + b_mid_ref[...]
    sig_two = sigmoid(pre_two)
    act_two = (pre_two * sig_two).astype(jnp.bfloat16)
    slope_two = sig_two * (1.0 + pre_two * (1.0 - sig_two))
    back_two = dot(column_cot, w_out_ref[...], NT)
    delta_two = (back_two * slope_two).astype(jnp.bfloat16)
    back_one = dot(delta_two, w_mid_ref[...], NT)
    delta_one = (back_one * slope_one).astype(jnp.bfloat16)
    back_norm = dot(delta_one, w_in_ref[...], NT)
    scaled = back_norm * gain
    grad_columns = inverse * scaled - inputs * (inverse * inverse * inverse) * jnp.mean(
        scaled * inputs, axis=1, keepdims=True
    )
    grad_columns = grad_columns.astype(jnp.bfloat16)
    back = dot(ana_ref[...], grad_columns, NN).astype(jnp.bfloat16)
    half = back.shape[1] // levels
    for j in range(levels):
        back_ref[0, j] = jnp.concatenate(
            [back[p * waves : (p + 1) * waves, j * half : (j + 1) * half] for p in range(2)],
            axis=1,
        )
    first, second = w_in_ref.size // 128, w_mid_ref.size // 128
    add_blocks(grads_ref, 0, dot(normed, delta_one, TN))
    add_blocks(grads_ref, first, dot(act_one, delta_two, TN))
    add_blocks(grads_ref, first + second, dot(act_two, column_cot, TN))
    small = (
        jnp.sum(back_norm * inputs * inverse, axis=0, keepdims=True),
        jnp.sum(delta_one.astype(jnp.float32), axis=0, keepdims=True),
        jnp.sum(delta_two.astype(jnp.float32), axis=0, keepdims=True),
    )
    at = 0
    for value in small:
        add_blocks(small_ref, at, value)
        at += value.shape[1] // 128


def column_call(recv, table, gain, w_in, b_in, w_mid, b_mid, w_out):
    kinds, members, levels, pairs, lanes = recv.shape
    bf16 = jnp.bfloat16
    waves, longitudes = table.shape
    params = (table, table.T, gain[None], w_in, b_in[None], w_mid, b_mid[None], w_out)
    whole = lambda a: pl.BlockSpec(a.shape, lambda b: (0,) * a.ndim)
    out = (
        jax.ShapeDtypeStruct((members, levels, pairs, lanes), bf16),
        jax.ShapeDtypeStruct(
            ((w_in.size + w_mid.size + w_out.size) // lanes, lanes), jnp.float32
        ),
        jax.ShapeDtypeStruct((16, lanes), jnp.float32),
    )
    return pl.pallas_call(
        column_kernel,
        grid=(members,),
        out_shape=out,
        in_specs=[
            pl.BlockSpec((kinds, 1, levels, pairs, lanes), lambda b: (0, b, 0, 0, 0))
        ]
        + [whole(a) for a in params],
        out_specs=[
            pl.BlockSpec((1, levels, pairs, lanes), lambda b: (b, 0, 0, 0)),
            whole(out[1]),
            whole(out[2]),
        ],
        scratch_shapes=[
            pltpu.VMEM((2 * longitudes, 2 * waves), bf16),
            pltpu.VMEM((2 * waves, 2 * longitudes), bf16),
        ],
        compiler_params=pltpu.CompilerParams(
            dimension_semantics=("arbitrary",), vmem_limit_bytes=58 * 1024 * 1024
        ),
        name="columns",
    )(recv, *params)


def local(
    n_lat, n_lev, spec_in, cotangent, legendre, quad_weights, wave_order, norm_gain, weight_in,
    bias_in, weight_mid, bias_mid, weight_out,
):
    bf16 = jnp.bfloat16
    n = n_lat * n_lev
    slots_here, degrees, members, lanes = spec_in.shape
    rows = NLAT // n
    own_waves = lax.dynamic_slice_in_dim(wave_order, lax.axis_index("lat") * slots_here, slots_here)
    living, shrink = spectral_masks(own_waves, degrees)
    basis_rows = jnp.where(living[:, :, None], legendre, jnp.zeros_like(legendre))
    table = fourier_tables(wave_order)
    lane = np.arange(lanes)
    apart = np.zeros((lanes, lanes), np.float32)
    apart[lane, (lane % 2) * (lanes // 2) + lane // 2] = 1.0
    apart = jnp.asarray(apart, bf16)

    pushed = (time_step * cotangent.astype(jnp.float32) * shrink[:, :, None, None]).astype(bf16)
    both = jnp.concatenate([spec_in, pushed], axis=2)
    both = jnp.einsum("slek,kq->sleq", both, apart, preferred_element_type=jnp.float32)
    fourier = jnp.einsum(
        "slt,sleq->setq", basis_rows, both.astype(bf16), preferred_element_type=jnp.float32
    )
    is_state = jnp.arange(2 * members) < members
    weights = jnp.where(is_state[:, None], 1.0, quad_weights[None, :])
    fourier = (fourier * weights[None, :, :, None]).astype(bf16)
    fourier = fourier.reshape(slots_here, 2 * members, n, rows, lanes)
    recv = exchange_out_call(fourier, n_lat, n_lev)
    recv = recv.reshape(2, members, n_lev, n_lat * slots_here * rows, lanes)
    back, grads, small = column_call(
        recv, table, norm_gain, weight_in, bias_in, weight_mid, bias_mid, weight_out
    )
    back = back.reshape(members, n_lev, n_lat * slots_here, rows, lanes)
    landed, total, small = exchange_back_call(back, grads, small, n_lat, n_lev)
    landed = landed.reshape(members, slots_here, n * rows, lanes)
    landed = jnp.einsum(
        "estq,kq->setk", landed, apart, preferred_element_type=jnp.float32
    ).astype(bf16)
    grad_spec = cotangent.astype(jnp.float32) * shrink[:, :, None, None] + jnp.einsum(
        "slt,setk->slek", basis_rows, landed, preferred_element_type=jnp.float32
    )
    factor = float(MEMBERS * NLAT * NLON) ** (-0.5)
    total = total.reshape(-1, lanes)
    out, at = [], 0
    for like in (weight_in, weight_mid, weight_out):
        size = like.size // lanes
        blocks = total[at : at + size].reshape(-1, like.shape[0], lanes)
        out.append(blocks.transpose(1, 0, 2).reshape(like.shape).astype(jnp.float32) * factor)
        at += size
    small = small.reshape(-1) * factor
    gain_end, in_end = norm_gain.size, norm_gain.size + bias_in.size
    return (
        grad_spec, small[:gain_end], out[0], small[gain_end:in_end], out[1],
        small[in_end : in_end + bias_mid.size], out[2],
    )


def solution(mesh):
    split = P("lat", None, None, "lev")
    placed = (split, split, P("lat", None, None)) + (P(),) * 8
    return jax.shard_map(
        functools.partial(local, mesh.shape["lat"], mesh.shape["lev"]),
        mesh=mesh,
        in_specs=placed,
        out_specs=(split,) + (P(),) * 6,
        check_vma=False,
    )
```

```python
import functools
import math

import jax
import jax.numpy as jnp
import numpy as np
from jax import lax
from jax.experimental import pallas as pl
from jax.experimental.pallas import tpu as pltpu
from jax.sharding import PartitionSpec as P

WAVES = 171
NLAT = 256
NLON = 512
MEMBERS = 4

time_step = 0.5
norm_eps = 1e-06
MESH = pl.DeviceIdType.MESH


def spectral_masks(waves_held, degree_count):
    degree = jnp.arange(degree_count, dtype=jnp.int32)
    living = (waves_held[:, None] <= degree[None, :]) & (waves_held[:, None] < WAVES)
    ratio = (degree * (degree + 1)).astype(jnp.float32) / float(WAVES * (WAVES - 1))
    factor = 1.0 / (1.0 + ratio * ratio)
    shrink = jnp.where(living, factor[None, :], jnp.zeros_like(factor)[None, :])
    return (living, shrink)


def fourier_tables(waves_all):
    longitude = jnp.arange(NLON, dtype=jnp.int32)
    phase_steps = waves_all[:, None] * longitude[None, :] % NLON
    angles = phase_steps.astype(jnp.float32) * (2.0 * math.pi / NLON)
    weight_scale = jnp.where(waves_all < WAVES, math.sqrt(2.0 / NLON), 0.0).astype(jnp.float32)[
        :, None
    ]
    table = jnp.concatenate(
        [jnp.cos(angles) * weight_scale, -jnp.sin(angles) * weight_scale], axis=0
    ).astype(jnp.bfloat16)
    return table


def part(value, size, of):
    return lax.rem(value // of, size)


def peer_at(step, i, j):
    away = lax.rem(step * 37, 128)
    z = lax.rem(i // 8 + lax.rem(away, 4), 4)
    y = lax.rem(part(i, 4, 2) + part(away, 4, 4), 4)
    x = lax.rem(lax.rem(i, 2) * 2 + j // 2 + part(away, 4, 16), 4)
    core = lax.rem(j + away // 64, 2)
    return z * 8 + y * 2 + x // 2, lax.rem(x, 2) * 2 + core


def chip_at(step, i, j):
    away = lax.rem(step * 37, 64)
    z = lax.rem(i // 8 + lax.rem(away, 4), 4)
    y = lax.rem(part(i, 4, 2) + part(away, 4, 4), 4)
    x = lax.rem(lax.rem(i, 2) * 2 + j // 2 + away // 16, 4)
    return z * 8 + y * 2 + x // 2, lax.rem(x, 2) * 2 + lax.rem(j, 2)


def send(src, dst, send_sem, recv_sem, peer):
    copy = pltpu.make_async_remote_copy(
        src_ref=src, dst_ref=dst, send_sem=send_sem, recv_sem=recv_sem,
        device_id=peer, device_id_type=MESH,
    )
    copy.start()
    return copy


def await_bytes(like, sem):
    pltpu.make_async_copy(like, like, sem).wait()


def dot(a, b, dims):
    return lax.dot_general(a, b, (dims, ((), ())), preferred_element_type=jnp.float32)


def sigmoid(z):
    return 0.5 * jnp.tanh(0.5 * z) + 0.5


def join_levels(parts):
    half = parts[0].shape[1] // 2
    rows = []
    for p in range(2):
        rows.append(
            jnp.concatenate([a[:, p * half : (p + 1) * half] for a in parts], axis=1)
        )
    return jnp.concatenate(rows, axis=0)


def one_of_two(shape, long_dim, which):
    long = lax.broadcasted_iota(jnp.int32, shape, long_dim)
    short = lax.broadcasted_iota(jnp.int32, shape, 1 - long_dim)
    return jnp.where(long == 2 * short + which, 1.0, 0.0).astype(jnp.bfloat16)


NN, NT, TN = (((1,), (0,)), ((1,), (1,)), ((0,), (0,)))


def add_blocks(ref, start, value):
    rows, lanes = value.shape[0], ref.shape[1]
    for b in range(value.shape[1] // lanes):
        ref[pl.ds(start + b * rows, rows)] += value[:, b * lanes : (b + 1) * lanes]


def column_work(
    state, cot, syn_ref, ana_ref, gain_ref, w_in_ref, b_in_ref, w_mid_ref, b_mid_ref, w_out_ref
):
    bf16 = jnp.bfloat16
    columns = dot(syn_ref[...], state, NN).astype(bf16)
    column_cot = dot(syn_ref[...], cot, NN).astype(bf16)
    gain = gain_ref[...]
    inputs = columns.astype(jnp.float32)
    inverse = lax.rsqrt(jnp.mean(inputs * inputs, axis=1, keepdims=True) + norm_eps)
    normed = (inputs * inverse * gain).astype(bf16)
    pre_one = dot(normed, w_in_ref[...], NN) + b_in_ref[...]
    sig_one = sigmoid(pre_one)
    act_one = (pre_one * sig_one).astype(bf16)
    slope_one = sig_one * (1.0 + pre_one * (1.0 - sig_one))
    pre_two = dot(act_one, w_mid_ref[...], NN) + b_mid_ref[...]
    sig_two = sigmoid(pre_two)
    act_two = (pre_two * sig_two).astype(bf16)
    slope_two = sig_two * (1.0 + pre_two * (1.0 - sig_two))
    back_two = dot(column_cot, w_out_ref[...], NT)
    delta_two = (back_two * slope_two).astype(bf16)
    back_one = dot(delta_two, w_mid_ref[...], NT)
    delta_one = (back_one * slope_one).astype(bf16)
    back_norm = dot(delta_one, w_in_ref[...], NT)
    scaled = back_norm * gain
    grad_columns = inverse * scaled - inputs * (inverse * inverse * inverse) * jnp.mean(
        scaled * inputs, axis=1, keepdims=True
    )
    back = dot(ana_ref[...], grad_columns.astype(bf16), NN).astype(bf16)
    gain_sum = jnp.sum(back_norm * inputs * inverse, axis=0, keepdims=True)
    return back, (normed, delta_one, act_one, delta_two, act_two, column_cot, gain_sum)


def whole_step(
    n, four_ref, table_ref, table_t_ref, gain_ref, w_in_ref, b_in_ref, w_mid_ref, b_mid_ref,
    w_out_ref, landed_ref, total_ref, small_total_ref,
    recv_ref, back_ref, syn_ref, ana_ref, grads_ref, small_ref,
    their_half, rs_src, rs_recv, ag_src, small_recv, small_sum,
    out_sems, arrive_sems, own_sems, pair_sems, back_sems, rs_sems, ag_sems, swap_sems,
    small_sems, small_back_sems, local_sems,
):
    i, j = lax.axis_index("lat"), lax.axis_index("lev")
    me = i * 4 + j
    core = lax.rem(j, 2)
    chip = i * 2 + j // 2
    chips = n // 2
    partner = (i, j + 1 - 2 * core)
    members, slots = landed_ref.shape[:2]
    levels = recv_ref.shape[2]
    waves, longitudes = table_ref.shape
    is_owner = me == 0

    def arriving(e):
        return recv_ref.at[e, :, j, pl.ds(i * slots, slots)]

    def start_out(e):
        def start(step, carry):
            peer = peer_at(step, i, j)
            send(
                four_ref.at[e, :, :, peer[0] * 4 + peer[1]], arriving(e),
                out_sems.at[0], arrive_sems.at[e], peer,
            )
            return carry

        pltpu.make_async_copy(four_ref.at[e, :, :, me], arriving(e), own_sems.at[e]).start()
        lax.fori_loop(1, n, start, 0)

    start_out(0)
    start_out(1)
    grads_ref[...] = jnp.zeros_like(grads_ref)
    small_ref[...] = jnp.zeros_like(small_ref)
    for r in range(2):
        span = pl.ds(r * longitudes, longitudes)
        syn_ref[span] = dot(
            table_t_ref[...], one_of_two((waves, 2 * waves), 1, r), NN
        ).astype(jnp.bfloat16)
        ana_ref[:, span] = dot(
            one_of_two((2 * waves, waves), 0, r), table_ref[...], NN
        ).astype(jnp.bfloat16)

    recv_rows = recv_ref.reshape(members, 2, levels, 2 * n // 4 * slots, recv_ref.shape[-1])
    back_rows = back_ref.reshape(members, levels, 2 * n // 4 * slots, back_ref.shape[-1])

    def member(e, carry):
        @pl.when(e < members - 2)
        def _():
            start_out(e + 2)

        pltpu.make_async_copy(four_ref.at[e, :, :, me], arriving(e), own_sems.at[e]).wait()
        await_bytes(four_ref.at[e, :, :, pl.ds(0, n - 1)], arrive_sems.at[e])
        state = join_levels([recv_rows[e, 0, k] for k in range(levels)])
        cot = join_levels([recv_rows[e, 1, k] for k in range(levels)])
        back, rest = column_work(
            state, cot, syn_ref, ana_ref, gain_ref, w_in_ref, b_in_ref, w_mid_ref, b_mid_ref,
            w_out_ref,
        )
        half = back.shape[1] // levels
        for k in range(levels):
            back_rows[e, k] = jnp.concatenate(
                [back[p * waves : (p + 1) * waves, k * half : (k + 1) * half] for p in range(2)],
                axis=1,
            )

        def start_back(step, carry):
            peer = peer_at(step, i, j)
            send(
                back_ref.at[e, peer[1], pl.ds(peer[0] * slots, slots)], landed_ref.at[e, :, me],
                back_sems.at[0], back_sems.at[1], peer,
            )
            return carry

        pltpu.make_async_copy(
            back_ref.at[e, j, pl.ds(i * slots, slots)], landed_ref.at[e, :, me],
            local_sems.at[1],
        ).start()
        lax.fori_loop(1, n, start_back, 0)

        normed, delta_one, act_one, delta_two, act_two, column_cot, gain_sum = rest
        first, second = w_in_ref.size // 128, w_mid_ref.size // 128
        add_blocks(grads_ref, 0, dot(normed, delta_one, TN))
        add_blocks(grads_ref, first, dot(act_one, delta_two, TN))
        add_blocks(grads_ref, first + second, dot(act_two, column_cot, TN))
        at = 0
        for value in (
            gain_sum,
            jnp.sum(delta_one.astype(jnp.float32), axis=0, keepdims=True),
            jnp.sum(delta_two.astype(jnp.float32), axis=0, keepdims=True),
        ):
            add_blocks(small_ref, at, value)
            at += value.shape[1] // 128
        return carry

    lax.fori_loop(0, members, member, 0)

    half_rows = their_half.shape[0]
    pair = send(
        grads_ref.at[pl.ds((1 - core) * half_rows, half_rows)], their_half,
        pair_sems.at[0], pair_sems.at[1], partner,
    )

    @pl.when(jnp.logical_not(is_owner))
    def _():
        send(small_ref, small_recv.at[me], small_sems.at[0], small_sems.at[1], (0, 0))

    pair.wait()
    mine = grads_ref[pl.ds(pl.multiple_of(core * half_rows, half_rows), half_rows)]
    rs_src[...] = (mine + their_half[...]).astype(rs_src.dtype).reshape(rs_src.shape)

    def start_rs(step, carry):
        peer = chip_at(step, i, j)
        send(
            rs_src.at[peer[0] * 2 + peer[1] // 2], rs_recv.at[chip],
            rs_sems.at[0], rs_sems.at[1], peer,
        )
        return carry

    lax.fori_loop(1, chips, start_rs, 0)

    @pl.when(is_owner)
    def _():
        small_recv[0] = small_ref[...]
        await_bytes(small_recv.at[pl.ds(0, n - 1)], small_sems.at[1])
        small_sum[...] = jnp.sum(small_recv[...], axis=0)

        def start_small(step, carry):
            peer = peer_at(step, i, j)
            send(
                small_sum, small_total_ref, small_back_sems.at[0], small_back_sems.at[1], peer
            )
            return carry

        lax.fori_loop(1, n, start_small, 0)
        mine = pltpu.make_async_copy(small_sum, small_total_ref, local_sems.at[2])
        mine.start()
        mine.wait()
        await_bytes(small_recv.at[pl.ds(0, n - 1)], small_back_sems.at[0])

    @pl.when(jnp.logical_not(is_owner))
    def _():
        await_bytes(small_ref, small_sems.at[0])

    rs_recv[chip] = rs_src[chip]
    await_bytes(rs_src.at[pl.ds(0, chips - 1)], rs_sems.at[1])
    ag_src[...] = jnp.sum(rs_recv[...].astype(jnp.float32), axis=0).astype(ag_src.dtype)

    def start_ag(step, carry):
        peer = chip_at(step, i, j)
        send(ag_src, total_ref.at[core, chip], ag_sems.at[0], ag_sems.at[1], peer)
        return carry

    lax.fori_loop(1, chips, start_ag, 0)
    mine = pltpu.make_async_copy(ag_src, total_ref.at[core, chip], local_sems.at[3])
    mine.start()
    mine.wait()
    await_bytes(rs_src.at[pl.ds(0, chips - 1)], rs_sems.at[0])
    await_bytes(rs_src.at[pl.ds(0, chips - 1)], ag_sems.at[1])
    swap = send(
        total_ref.at[core], total_ref.at[core], swap_sems.at[0], swap_sems.at[1], partner
    )
    await_bytes(rs_src.at[pl.ds(0, chips - 1)], ag_sems.at[0])
    await_bytes(landed_ref.at[:, :, 0], local_sems.at[1])
    many = landed_ref.at[:, :, pl.ds(0, n - 1)]
    await_bytes(many, back_sems.at[0])
    await_bytes(many, back_sems.at[1])
    await_bytes(four_ref.at[:, :, :, pl.ds(0, n - 1)], out_sems.at[0])

    @pl.when(jnp.logical_not(is_owner))
    def _():
        await_bytes(small_ref, small_back_sems.at[1])

    swap.wait()


def whole_step_call(four, table, gain, w_in, b_in, w_mid, b_mid, w_out, n_lat, n_lev):
    members, kinds, slots, n, two, lanes = four.shape
    bf16, f32 = jnp.bfloat16, jnp.float32
    waves, longitudes = table.shape
    params = (table, table.T, gain[None], w_in, b_in[None], w_mid, b_mid[None], w_out)
    chips = n // 2
    grad_rows = (w_in.size + w_mid.size + w_out.size) // lanes
    half = grad_rows // 2
    slices = (chips, half // chips, lanes)
    small = (16, lanes)
    dma = pltpu.SemaphoreType.DMA
    return pl.pallas_call(
        functools.partial(whole_step, n),
        out_shape=(
            jax.ShapeDtypeStruct((members, slots, n, two, lanes), bf16),
            jax.ShapeDtypeStruct((2,) + slices, bf16),
            jax.ShapeDtypeStruct(small, f32),
        ),
        in_specs=[pl.BlockSpec(memory_space=pl.ANY)]
        + [pl.BlockSpec(memory_space=pltpu.VMEM)] * len(params),
        out_specs=[pl.BlockSpec(memory_space=pl.ANY)] * 3,
        scratch_shapes=[
            pltpu.VMEM((members, kinds, n_lev, n_lat * slots, two, lanes), bf16),
            pltpu.VMEM((members, n_lev, n_lat * slots, two, lanes), bf16),
            pltpu.VMEM((2 * longitudes, 2 * waves), bf16),
            pltpu.VMEM((2 * waves, 2 * longitudes), bf16),
            pltpu.VMEM((grad_rows, lanes), f32),
            pltpu.VMEM(small, f32),
            pltpu.VMEM((half, lanes), f32),
            pltpu.VMEM(slices, bf16),
            pltpu.VMEM(slices, bf16),
            pltpu.VMEM(slices[1:], bf16),
            pltpu.VMEM((n,) + small, f32),
            pltpu.VMEM(small, f32),
            dma((1,)),
            dma((members,)),
            dma((members,)),
        ]
        + [dma((2,))] * 7
        + [dma((4,))],
        compiler_params=pltpu.CompilerParams(
            has_side_effects=True, vmem_limit_bytes=60 * 1024 * 1024
        ),
        name="whole_step",
    )(four, *params)


def local(
    n_lat, n_lev, spec_in, cotangent, legendre, quad_weights, wave_order, norm_gain, weight_in,
    bias_in, weight_mid, bias_mid, weight_out,
):
    bf16 = jnp.bfloat16
    n = n_lat * n_lev
    slots_here, degrees, members, lanes = spec_in.shape
    rows = NLAT // n
    own_waves = lax.dynamic_slice_in_dim(wave_order, lax.axis_index("lat") * slots_here, slots_here)
    living, shrink = spectral_masks(own_waves, degrees)
    basis_rows = jnp.where(living[:, :, None], legendre, jnp.zeros_like(legendre))
    table = fourier_tables(wave_order)
    lane = np.arange(lanes)
    apart = np.zeros((lanes, lanes), np.float32)
    apart[lane, (lane % 2) * (lanes // 2) + lane // 2] = 1.0
    apart = jnp.asarray(apart, bf16)

    pushed = (time_step * cotangent.astype(jnp.float32) * shrink[:, :, None, None]).astype(bf16)
    both = jnp.stack([spec_in, pushed], axis=3)
    both = jnp.einsum("slehk,kq->slehq", both, apart, preferred_element_type=jnp.float32)
    fourier = jnp.einsum(
        "slt,slehq->sehtq", basis_rows, both.astype(bf16), preferred_element_type=jnp.float32
    )
    weights = jnp.stack([jnp.ones_like(quad_weights), quad_weights])
    fourier = (fourier * weights[None, None, :, :, None]).astype(bf16)
    fourier = fourier.transpose(1, 2, 0, 3, 4)
    fourier = fourier.reshape(members, 2, slots_here, n, rows, lanes)
    landed, total, small = whole_step_call(
        fourier, table, norm_gain, weight_in, bias_in, weight_mid, bias_mid, weight_out,
        n_lat, n_lev,
    )
    landed = landed.reshape(members, slots_here, n * rows, lanes)
    landed = jnp.einsum(
        "estq,kq->setk", landed, apart, preferred_element_type=jnp.float32
    ).astype(bf16)
    grad_spec = cotangent.astype(jnp.float32) * shrink[:, :, None, None] + jnp.einsum(
        "slt,setk->slek", basis_rows, landed, preferred_element_type=jnp.float32
    )
    factor = float(MEMBERS * NLAT * NLON) ** (-0.5)
    total = total.reshape(-1, lanes)
    out, at = [], 0
    for like in (weight_in, weight_mid, weight_out):
        size = like.size // lanes
        blocks = total[at : at + size].reshape(-1, like.shape[0], lanes)
        out.append(blocks.transpose(1, 0, 2).reshape(like.shape).astype(jnp.float32) * factor)
        at += size
    small = small.reshape(-1) * factor
    gain_end, in_end = norm_gain.size, norm_gain.size + bias_in.size
    return (
        grad_spec, small[:gain_end], out[0], small[gain_end:in_end], out[1],
        small[in_end : in_end + bias_mid.size], out[2],
    )


def solution(mesh):
    split = P("lat", None, None, "lev")
    placed = (split, split, P("lat", None, None)) + (P(),) * 8
    return jax.shard_map(
        functools.partial(local, mesh.shape["lat"], mesh.shape["lev"]),
        mesh=mesh,
        in_specs=placed,
        out_specs=(split,) + (P(),) * 6,
        check_vma=False,
    )
```

```python
import functools
import math

import jax
import jax.numpy as jnp
import numpy as np
from jax import lax
from jax.experimental import pallas as pl
from jax.experimental.pallas import tpu as pltpu
from jax.sharding import PartitionSpec as P

WAVES = 171
NLAT = 256
NLON = 512
MEMBERS = 4

time_step = 0.5
norm_eps = 1e-06
MESH = pl.DeviceIdType.MESH


def spectral_masks(waves_held, degree_count):
    degree = jnp.arange(degree_count, dtype=jnp.int32)
    living = (waves_held[:, None] <= degree[None, :]) & (waves_held[:, None] < WAVES)
    ratio = (degree * (degree + 1)).astype(jnp.float32) / float(WAVES * (WAVES - 1))
    factor = 1.0 / (1.0 + ratio * ratio)
    shrink = jnp.where(living, factor[None, :], jnp.zeros_like(factor)[None, :])
    return (living, shrink)


def fourier_table(waves_all):
    shape = (NLON, waves_all.shape[1])
    longitude = lax.broadcasted_iota(jnp.int32, shape, 0)
    phase_steps = jnp.bitwise_and(waves_all * longitude, NLON - 1)
    angles = phase_steps.astype(jnp.float32) * (2.0 * math.pi / NLON)
    scale = jnp.where(waves_all < WAVES, math.sqrt(2.0 / NLON), 0.0).astype(jnp.float32)
    return jnp.concatenate(
        [jnp.cos(angles) * scale, -jnp.sin(angles) * scale], axis=1
    ).astype(jnp.bfloat16)


AROUND = (
    (1, 2), (2, 1), (0, 3), (3, 0), (1, 1), (2, 3), (0, 1), (3, 2), (1, 0), (2, 2), (0, 2),
    (3, 1), (2, 0), (1, 3), (3, 3),
)


def each_chip(i, j, visit):
    z = [lax.rem(i // 8 + d, 4) * 8 for d in range(4)]
    y = [lax.rem(lax.rem(i // 2, 4) + d, 4) * 2 for d in range(4)]
    x = lax.rem(i, 2) * 2 + j // 2

    def along_x(d):
        to = lax.rem(x + d, 4)
        return to // 2, lax.rem(to, 2) * 2

    for d in (1, 2, 3):
        high, low = along_x(d)
        visit(z[0] + y[0] + high, low)

    def turn(a, carry):
        across = [along_x(a + d) for d in range(4)]
        for at, (dz, dy) in enumerate(AROUND):
            high, low = across[at % 4]
            visit(z[dz] + y[dy] + high, low)
        return carry

    lax.fori_loop(0, 4, turn, 0)


def each_peer(i, j, visit):
    visit(i, j + 1 - 2 * lax.rem(j, 2))

    def both(lat, low):
        visit(lat, low)
        visit(lat, low + 1)

    each_chip(i, j, both)


def send(src, dst, send_sem, recv_sem, peer):
    copy = pltpu.make_async_remote_copy(
        src_ref=src, dst_ref=dst, send_sem=send_sem, recv_sem=recv_sem,
        device_id=peer, device_id_type=MESH,
    )
    copy.start()
    return copy


def await_bytes(like, sem):
    pltpu.make_async_copy(like, like, sem).wait()


def dot(a, b, dims):
    return lax.dot_general(a, b, (dims, ((), ())), preferred_element_type=jnp.float32)


def sigmoid(z):
    return 0.5 * jnp.tanh(0.5 * z) + 0.5


def join_levels(parts):
    half = parts[0].shape[1] // 2
    rows = []
    for p in range(2):
        rows.append(
            jnp.concatenate([a[:, p * half : (p + 1) * half] for a in parts], axis=1)
        )
    return jnp.concatenate(rows, axis=0)


def one_of_two(shape, long_dim, which):
    long = lax.broadcasted_iota(jnp.int32, shape, long_dim)
    short = lax.broadcasted_iota(jnp.int32, shape, 1 - long_dim)
    return jnp.where(long == 2 * short + which, 1.0, 0.0).astype(jnp.bfloat16)


NN, NT, TN = (((1,), (0,)), ((1,), (1,)), ((0,), (0,)))


def add_blocks(ref, start, value):
    rows, lanes = value.shape[0], ref.shape[1]
    for b in range(value.shape[1] // lanes):
        ref[pl.ds(start + b * rows, rows)] += value[:, b * lanes : (b + 1) * lanes]


def column_work(
    state, cot, syn_ref, ana_ref, gain_ref, w_in_ref, b_in_ref, w_mid_ref, b_mid_ref, w_out_ref
):
    bf16 = jnp.bfloat16
    columns = dot(syn_ref[...], state, NN).astype(bf16)
    column_cot = dot(syn_ref[...], cot, NN).astype(bf16)
    gain = gain_ref[...]
    inputs = columns.astype(jnp.float32)
    inverse = lax.rsqrt(jnp.mean(inputs * inputs, axis=1, keepdims=True) + norm_eps)
    normed = (inputs * inverse * gain).astype(bf16)
    pre_one = dot(normed, w_in_ref[...], NN) + b_in_ref[...]
    sig_one = sigmoid(pre_one)
    act_one = (pre_one * sig_one).astype(bf16)
    slope_one = sig_one * (1.0 + pre_one * (1.0 - sig_one))
    pre_two = dot(act_one, w_mid_ref[...], NN) + b_mid_ref[...]
    sig_two = sigmoid(pre_two)
    act_two = (pre_two * sig_two).astype(bf16)
    slope_two = sig_two * (1.0 + pre_two * (1.0 - sig_two))
    back_two = dot(column_cot, w_out_ref[...], NT)
    delta_two = (back_two * slope_two).astype(bf16)
    back_one = dot(delta_two, w_mid_ref[...], NT)
    delta_one = (back_one * slope_one).astype(bf16)
    back_norm = dot(delta_one, w_in_ref[...], NT)
    scaled = back_norm * gain
    grad_columns = inverse * scaled - inputs * (inverse * inverse * inverse) * jnp.mean(
        scaled * inputs, axis=1, keepdims=True
    )
    back = dot(ana_ref[...], grad_columns.astype(bf16), NN).astype(bf16)
    gain_sum = jnp.sum(back_norm * inputs * inverse, axis=0, keepdims=True)
    return back, (normed, delta_one, act_one, delta_two, act_two, column_cot, gain_sum)


def whole_step(
    n, four_ref, waves_ref, gain_ref, w_in_ref, b_in_ref, w_mid_ref, b_mid_ref,
    w_out_ref, landed_ref, total_ref, small_total_ref,
    recv_ref, back_ref, syn_ref, ana_ref, grads_ref, small_ref,
    their_half, rs_src, rs_recv, ag_src, small_recv, small_sum,
    out_sems, arrive_sems, own_sems, pair_sems, back_sems, rs_sems, ag_sems, swap_sems,
    small_sems, small_back_sems, local_sems,
):
    i, j = lax.axis_index("lat"), lax.axis_index("lev")
    me = i * 4 + j
    core = lax.rem(j, 2)
    chip = i * 2 + j // 2
    chips = n // 2
    partner = (i, j + 1 - 2 * core)
    members, slots = landed_ref.shape[:2]
    levels = recv_ref.shape[2]
    waves, longitudes = 2 * waves_ref.shape[1], NLON
    is_owner = me == 0

    def arriving(e):
        return recv_ref.at[e, :, j, pl.ds(i * slots, slots)]

    def start_out(e):
        def visit(lat, lev):
            send(
                four_ref.at[e, :, :, lat * 4 + lev], arriving(e),
                out_sems.at[0], arrive_sems.at[e], (lat, lev),
            )

        pltpu.make_async_copy(four_ref.at[e, :, :, me], arriving(e), own_sems.at[e]).start()
        each_peer(i, j, visit)

    start_out(0)
    start_out(1)
    grads_ref[...] = jnp.zeros_like(grads_ref)
    small_ref[...] = jnp.zeros_like(small_ref)
    table = fourier_table(waves_ref[...])
    for r in range(2):
        span = pl.ds(r * longitudes, longitudes)
        syn_ref[span] = dot(table, one_of_two((waves, 2 * waves), 1, r), NN).astype(jnp.bfloat16)
        ana_ref[:, span] = dot(one_of_two((2 * waves, waves), 0, r), table, NT).astype(
            jnp.bfloat16
        )

    recv_rows = recv_ref.reshape(members, 2, levels, 2 * n // 4 * slots, recv_ref.shape[-1])
    back_rows = back_ref.reshape(members, levels, 2 * n // 4 * slots, back_ref.shape[-1])

    def member(e, carry):
        @pl.when(e < members - 2)
        def _():
            start_out(e + 2)

        pltpu.make_async_copy(four_ref.at[e, :, :, me], arriving(e), own_sems.at[e]).wait()
        await_bytes(four_ref.at[e, :, :, pl.ds(0, n - 1)], arrive_sems.at[e])
        state = join_levels([recv_rows[e, 0, k] for k in range(levels)])
        cot = join_levels([recv_rows[e, 1, k] for k in range(levels)])
        back, rest = column_work(
            state, cot, syn_ref, ana_ref, gain_ref, w_in_ref, b_in_ref, w_mid_ref, b_mid_ref,
            w_out_ref,
        )
        half = back.shape[1] // levels
        for k in range(levels):
            back_rows[e, k] = jnp.concatenate(
                [back[p * waves : (p + 1) * waves, k * half : (k + 1) * half] for p in range(2)],
                axis=1,
            )

        def visit(lat, lev):
            send(
                back_ref.at[e, lev, pl.ds(lat * slots, slots)], landed_ref.at[e, :, me],
                back_sems.at[0], back_sems.at[1], (lat, lev),
            )

        pltpu.make_async_copy(
            back_ref.at[e, j, pl.ds(i * slots, slots)], landed_ref.at[e, :, me],
            local_sems.at[1],
        ).start()
        each_peer(i, j, visit)

        normed, delta_one, act_one, delta_two, act_two, column_cot, gain_sum = rest
        first, second = w_in_ref.size // 128, w_mid_ref.size // 128
        add_blocks(grads_ref, 0, dot(normed, delta_one, TN))
        add_blocks(grads_ref, first, dot(act_one, delta_two, TN))
        add_blocks(grads_ref, first + second, dot(act_two, column_cot, TN))
        at = 0
        for value in (
            gain_sum,
            jnp.sum(delta_one.astype(jnp.float32), axis=0, keepdims=True),
            jnp.sum(delta_two.astype(jnp.float32), axis=0, keepdims=True),
        ):
            add_blocks(small_ref, at, value)
            at += value.shape[1] // 128
        return carry

    lax.fori_loop(0, members, member, 0)

    half_rows = their_half.shape[0]
    pair = send(
        grads_ref.at[pl.ds((1 - core) * half_rows, half_rows)], their_half,
        pair_sems.at[0], pair_sems.at[1], partner,
    )

    @pl.when(jnp.logical_not(is_owner))
    def _():
        send(small_ref, small_recv.at[me], small_sems.at[0], small_sems.at[1], (0, 0))

    pair.wait()
    mine = grads_ref[pl.ds(pl.multiple_of(core * half_rows, half_rows), half_rows)]
    rs_src[...] = (mine + their_half[...]).astype(rs_src.dtype).reshape(rs_src.shape)

    def visit_rs(lat, low):
        send(
            rs_src.at[lat * 2 + low // 2], rs_recv.at[chip],
            rs_sems.at[0], rs_sems.at[1], (lat, low + core),
        )

    each_chip(i, j, visit_rs)

    @pl.when(is_owner)
    def _():
        small_recv[0] = small_ref[...]
        await_bytes(small_recv.at[pl.ds(0, n - 1)], small_sems.at[1])
        small_sum[...] = jnp.sum(small_recv[...], axis=0)

        def visit_small(lat, lev):
            send(
                small_sum, small_total_ref, small_back_sems.at[0], small_back_sems.at[1],
                (lat, lev),
            )

        each_peer(i, j, visit_small)
        mine = pltpu.make_async_copy(small_sum, small_total_ref, local_sems.at[2])
        mine.start()
        mine.wait()
        await_bytes(small_recv.at[pl.ds(0, n - 1)], small_back_sems.at[0])

    @pl.when(jnp.logical_not(is_owner))
    def _():
        await_bytes(small_ref, small_sems.at[0])

    rs_recv[chip] = rs_src[chip]
    await_bytes(rs_src.at[pl.ds(0, chips - 1)], rs_sems.at[1])
    ag_src[...] = jnp.sum(rs_recv[...].astype(jnp.float32), axis=0).astype(ag_src.dtype)

    def visit_ag(lat, low):
        send(
            ag_src, total_ref.at[core, chip], ag_sems.at[0], ag_sems.at[1], (lat, low + core)
        )

    each_chip(i, j, visit_ag)
    mine = pltpu.make_async_copy(ag_src, total_ref.at[core, chip], local_sems.at[3])
    mine.start()
    mine.wait()
    await_bytes(rs_src.at[pl.ds(0, chips - 1)], rs_sems.at[0])
    await_bytes(rs_src.at[pl.ds(0, chips - 1)], ag_sems.at[1])
    swap = send(
        total_ref.at[core], total_ref.at[core], swap_sems.at[0], swap_sems.at[1], partner
    )
    await_bytes(rs_src.at[pl.ds(0, chips - 1)], ag_sems.at[0])
    await_bytes(landed_ref.at[:, :, 0], local_sems.at[1])
    many = landed_ref.at[:, :, pl.ds(0, n - 1)]
    await_bytes(many, back_sems.at[0])
    await_bytes(many, back_sems.at[1])
    await_bytes(four_ref.at[:, :, :, pl.ds(0, n - 1)], out_sems.at[0])

    @pl.when(jnp.logical_not(is_owner))
    def _():
        await_bytes(small_ref, small_back_sems.at[1])

    swap.wait()


def whole_step_call(four, waves_all, gain, w_in, b_in, w_mid, b_mid, w_out, n_lat, n_lev):
    members, kinds, slots, n, two, lanes = four.shape
    bf16, f32 = jnp.bfloat16, jnp.float32
    waves, longitudes = 2 * waves_all.shape[0], NLON
    params = (waves_all[None], gain[None], w_in, b_in[None], w_mid, b_mid[None], w_out)
    chips = n // 2
    grad_rows = (w_in.size + w_mid.size + w_out.size) // lanes
    half = grad_rows // 2
    slices = (chips, half // chips, lanes)
    small = (16, lanes)
    dma = pltpu.SemaphoreType.DMA
    return pl.pallas_call(
        functools.partial(whole_step, n),
        out_shape=(
            jax.ShapeDtypeStruct((members, slots, n, two, lanes), bf16),
            jax.ShapeDtypeStruct((2,) + slices, bf16),
            jax.ShapeDtypeStruct(small, f32),
        ),
        in_specs=[pl.BlockSpec(memory_space=pl.ANY)]
        + [pl.BlockSpec(memory_space=pltpu.VMEM)] * len(params),
        out_specs=[pl.BlockSpec(memory_space=pl.ANY)] * 3,
        scratch_shapes=[
            pltpu.VMEM((members, kinds, n_lev, n_lat * slots, two, lanes), bf16),
            pltpu.VMEM((members, n_lev, n_lat * slots, two, lanes), bf16),
            pltpu.VMEM((2 * longitudes, 2 * waves), bf16),
            pltpu.VMEM((2 * waves, 2 * longitudes), bf16),
            pltpu.VMEM((grad_rows, lanes), f32),
            pltpu.VMEM(small, f32),
            pltpu.VMEM((half, lanes), f32),
            pltpu.VMEM(slices, bf16),
            pltpu.VMEM(slices, bf16),
            pltpu.VMEM(slices[1:], bf16),
            pltpu.VMEM((n,) + small, f32),
            pltpu.VMEM(small, f32),
            dma((1,)),
            dma((members,)),
            dma((members,)),
        ]
        + [dma((2,))] * 7
        + [dma((4,))],
        compiler_params=pltpu.CompilerParams(
            has_side_effects=True, vmem_limit_bytes=60 * 1024 * 1024
        ),
        name="whole_step",
    )(four, *params)


def local(
    n_lat, n_lev, spec_in, cotangent, legendre, quad_weights, wave_order, norm_gain, weight_in,
    bias_in, weight_mid, bias_mid, weight_out,
):
    bf16 = jnp.bfloat16
    n = n_lat * n_lev
    slots_here, degrees, members, lanes = spec_in.shape
    rows = NLAT // n
    own_waves = lax.dynamic_slice_in_dim(wave_order, lax.axis_index("lat") * slots_here, slots_here)
    living, shrink = spectral_masks(own_waves, degrees)
    basis_rows = jnp.where(living[:, :, None], legendre, jnp.zeros_like(legendre))
    lane = np.arange(lanes)
    apart = np.zeros((lanes, lanes), np.float32)
    apart[lane, (lane % 2) * (lanes // 2) + lane // 2] = 1.0
    apart = jnp.asarray(apart, bf16)

    pushed = (time_step * cotangent.astype(jnp.float32) * shrink[:, :, None, None]).astype(bf16)
    both = jnp.stack([spec_in, pushed], axis=3)
    both = jnp.einsum("slehk,kq->slehq", both, apart, preferred_element_type=jnp.float32)
    fourier = jnp.einsum(
        "slt,slehq->sehtq", basis_rows, both.astype(bf16), preferred_element_type=jnp.float32
    )
    weights = jnp.stack([jnp.ones_like(quad_weights), quad_weights])
    fourier = (fourier * weights[None, None, :, :, None]).astype(bf16)
    fourier = fourier.transpose(1, 2, 0, 3, 4)
    fourier = fourier.reshape(members, 2, slots_here, n, rows, lanes)
    landed, total, small = whole_step_call(
        fourier, wave_order, norm_gain, weight_in, bias_in, weight_mid, bias_mid, weight_out,
        n_lat, n_lev,
    )
    landed = landed.reshape(members, slots_here, n * rows, lanes)
    landed = jnp.einsum(
        "estq,kq->setk", landed, apart, preferred_element_type=jnp.float32
    ).astype(bf16)
    grad_spec = cotangent.astype(jnp.float32) * shrink[:, :, None, None] + jnp.einsum(
        "slt,setk->slek", basis_rows, landed, preferred_element_type=jnp.float32
    )
    factor = float(MEMBERS * NLAT * NLON) ** (-0.5)
    total = total.reshape(-1, lanes)
    out, at = [], 0
    for like in (weight_in, weight_mid, weight_out):
        size = like.size // lanes
        blocks = total[at : at + size].reshape(-1, like.shape[0], lanes)
        out.append(blocks.transpose(1, 0, 2).reshape(like.shape).astype(jnp.float32) * factor)
        at += size
    small = small.reshape(-1) * factor
    gain_end, in_end = norm_gain.size, norm_gain.size + bias_in.size
    return (
        grad_spec, small[:gain_end], out[0], small[gain_end:in_end], out[1],
        small[in_end : in_end + bias_mid.size], out[2],
    )


def solution(mesh):
    split = P("lat", None, None, "lev")
    placed = (split, split, P("lat", None, None)) + (P(),) * 8
    return jax.shard_map(
        functools.partial(local, mesh.shape["lat"], mesh.shape["lev"]),
        mesh=mesh,
        in_specs=placed,
        out_specs=(split,) + (P(),) * 6,
        check_vma=False,
    )
```

```python
import functools
import math

import jax
import jax.numpy as jnp
import numpy as np
from jax import lax
from jax.experimental import pallas as pl
from jax.experimental.pallas import tpu as pltpu
from jax.sharding import PartitionSpec as P

WAVES = 171
NLAT = 256
NLON = 512
MEMBERS = 4

time_step = 0.5
norm_eps = 1e-06
MESH = pl.DeviceIdType.MESH


def spectral_masks(waves_held, degree_count):
    degree = jnp.arange(degree_count, dtype=jnp.int32)
    living = (waves_held[:, None] <= degree[None, :]) & (waves_held[:, None] < WAVES)
    ratio = (degree * (degree + 1)).astype(jnp.float32) / float(WAVES * (WAVES - 1))
    factor = 1.0 / (1.0 + ratio * ratio)
    shrink = jnp.where(living, factor[None, :], jnp.zeros_like(factor)[None, :])
    return (living, shrink)


def fourier_table(waves_all):
    shape = (NLON, waves_all.shape[1])
    longitude = lax.broadcasted_iota(jnp.int32, shape, 0)
    phase_steps = jnp.bitwise_and(waves_all * longitude, NLON - 1)
    angles = phase_steps.astype(jnp.float32) * (2.0 * math.pi / NLON)
    scale = jnp.where(waves_all < WAVES, math.sqrt(2.0 / NLON), 0.0).astype(jnp.float32)
    return jnp.concatenate(
        [jnp.cos(angles) * scale, -jnp.sin(angles) * scale], axis=1
    ).astype(jnp.bfloat16)


AROUND = (
    (1, 2), (2, 1), (0, 3), (3, 0), (1, 1), (2, 3), (0, 1), (3, 2), (1, 0), (2, 2), (0, 2),
    (3, 1), (2, 0), (1, 3), (3, 3),
)


def each_chip(i, j, visit):
    z = [lax.rem(i // 8 + d, 4) * 8 for d in range(4)]
    y = [lax.rem(lax.rem(i // 2, 4) + d, 4) * 2 for d in range(4)]
    x = lax.rem(i, 2) * 2 + j // 2

    def along_x(d):
        to = lax.rem(x + d, 4)
        return to // 2, lax.rem(to, 2) * 2

    for d in (1, 2, 3):
        high, low = along_x(d)
        visit(z[0] + y[0] + high, low)

    def turn(a, carry):
        across = [along_x(a + d) for d in range(4)]
        for at, (dz, dy) in enumerate(AROUND):
            high, low = across[at % 4]
            visit(z[dz] + y[dy] + high, low)
        return carry

    lax.fori_loop(0, 4, turn, 0)


def each_peer(i, j, visit):
    visit(i, j + 1 - 2 * lax.rem(j, 2))

    def both(lat, low):
        visit(lat, low)
        visit(lat, low + 1)

    each_chip(i, j, both)


def send(src, dst, send_sem, recv_sem, peer):
    copy = pltpu.make_async_remote_copy(
        src_ref=src, dst_ref=dst, send_sem=send_sem, recv_sem=recv_sem,
        device_id=peer, device_id_type=MESH,
    )
    copy.start()
    return copy


def await_bytes(like, sem):
    pltpu.make_async_copy(like, like, sem).wait()


def dot(a, b, dims):
    return lax.dot_general(a, b, (dims, ((), ())), preferred_element_type=jnp.float32)


def sigmoid(z):
    return 0.5 * jnp.tanh(0.5 * z) + 0.5


def join_levels(parts):
    half = parts[0].shape[1] // 2
    rows = []
    for p in range(2):
        rows.append(
            jnp.concatenate([a[:, p * half : (p + 1) * half] for a in parts], axis=1)
        )
    return jnp.concatenate(rows, axis=0)


def one_of_two(shape, long_dim, which):
    long = lax.broadcasted_iota(jnp.int32, shape, long_dim)
    short = lax.broadcasted_iota(jnp.int32, shape, 1 - long_dim)
    return jnp.where(long == 2 * short + which, 1.0, 0.0).astype(jnp.bfloat16)


NN, NT, TN = (((1,), (0,)), ((1,), (1,)), ((0,), (0,)))


def add_blocks(ref, start, value):
    rows, lanes = value.shape[0], ref.shape[1]
    for b in range(value.shape[1] // lanes):
        ref[pl.ds(start + b * rows, rows)] += value[:, b * lanes : (b + 1) * lanes]


def column_work(
    state, cot, syn_ref, ana_ref, gain_ref, w_in_ref, b_in_ref, w_mid_ref, b_mid_ref, w_out_ref
):
    bf16 = jnp.bfloat16
    columns = dot(syn_ref[...], state, NN).astype(bf16)
    column_cot = dot(syn_ref[...], cot, NN).astype(bf16)
    gain = gain_ref[...]
    inputs = columns.astype(jnp.float32)
    inverse = lax.rsqrt(jnp.mean(inputs * inputs, axis=1, keepdims=True) + norm_eps)
    normed = (inputs * inverse * gain).astype(bf16)
    pre_one = dot(normed, w_in_ref[...], NN) + b_in_ref[...]
    sig_one = sigmoid(pre_one)
    act_one = (pre_one * sig_one).astype(bf16)
    slope_one = sig_one * (1.0 + pre_one * (1.0 - sig_one))
    pre_two = dot(act_one, w_mid_ref[...], NN) + b_mid_ref[...]
    sig_two = sigmoid(pre_two)
    act_two = (pre_two * sig_two).astype(bf16)
    slope_two = sig_two * (1.0 + pre_two * (1.0 - sig_two))
    back_two = dot(column_cot, w_out_ref[...], NT)
    delta_two = (back_two * slope_two).astype(bf16)
    back_one = dot(delta_two, w_mid_ref[...], NT)
    delta_one = (back_one * slope_one).astype(bf16)
    back_norm = dot(delta_one, w_in_ref[...], NT)
    scaled = back_norm * gain
    grad_columns = inverse * scaled - inputs * (inverse * inverse * inverse) * jnp.mean(
        scaled * inputs, axis=1, keepdims=True
    )
    back = dot(ana_ref[...], grad_columns.astype(bf16), NN).astype(bf16)
    gain_sum = jnp.sum(back_norm * inputs * inverse, axis=0, keepdims=True)
    return back, (normed, delta_one, act_one, delta_two, act_two, column_cot, gain_sum)


def whole_step(
    n, four_ref, waves_ref, gain_ref, w_in_ref, b_in_ref, w_mid_ref, b_mid_ref,
    w_out_ref, landed_ref, g_in_ref, g_mid_ref, g_out_ref, g_gain_ref, g_b_in_ref, g_b_mid_ref,
    recv_ref, back_ref, syn_ref, ana_ref, grads_ref, small_ref,
    their_half, their_small, rs_src, rs_recv, ag_src, total_ref, small_src, small_recv,
    small_total, out_sems, arrive_sems, own_sems, pair_sems, back_sems, rs_sems, ag_sems,
    swap_sems, small_sems, small_pair_sems, small_swap_sems, local_sems,
):
    i, j = lax.axis_index("lat"), lax.axis_index("lev")
    me = i * 4 + j
    core = lax.rem(j, 2)
    chip = i * 2 + j // 2
    chips = n // 2
    partner = (i, j + 1 - 2 * core)
    members, slots = landed_ref.shape[:2]
    levels = recv_ref.shape[2]
    waves, longitudes = 2 * waves_ref.shape[1], NLON

    def arriving(e):
        return recv_ref.at[e, :, j, pl.ds(i * slots, slots)]

    def start_out(e):
        def visit(lat, lev):
            send(
                four_ref.at[e, :, :, lat * 4 + lev], arriving(e),
                out_sems.at[0], arrive_sems.at[e], (lat, lev),
            )

        pltpu.make_async_copy(four_ref.at[e, :, :, me], arriving(e), own_sems.at[e]).start()
        each_peer(i, j, visit)

    start_out(0)
    start_out(1)
    grads_ref[...] = jnp.zeros_like(grads_ref)
    small_ref[...] = jnp.zeros_like(small_ref)
    table = fourier_table(waves_ref[...])
    for r in range(2):
        span = pl.ds(r * longitudes, longitudes)
        syn_ref[span] = dot(table, one_of_two((waves, 2 * waves), 1, r), NN).astype(jnp.bfloat16)
        ana_ref[:, span] = dot(one_of_two((2 * waves, waves), 0, r), table, NT).astype(
            jnp.bfloat16
        )

    def start_back(e):
        def visit(lat, lev):
            send(
                back_ref.at[e, lev, pl.ds(lat * slots, slots)], landed_ref.at[e, :, me],
                back_sems.at[0], back_sems.at[1], (lat, lev),
            )

        pltpu.make_async_copy(
            back_ref.at[e, j, pl.ds(i * slots, slots)], landed_ref.at[e, :, me],
            local_sems.at[0],
        ).start()
        each_peer(i, j, visit)

    recv_rows = recv_ref.reshape(members, 2, levels, 2 * n // 4 * slots, recv_ref.shape[-1])
    back_rows = back_ref.reshape(members, levels, 2 * n // 4 * slots, back_ref.shape[-1])

    def member(e, carry):
        @pl.when(e < members - 2)
        def _():
            start_out(e + 2)

        pltpu.make_async_copy(four_ref.at[e, :, :, me], arriving(e), own_sems.at[e]).wait()
        await_bytes(four_ref.at[e, :, :, pl.ds(0, n - 1)], arrive_sems.at[e])
        state = join_levels([recv_rows[e, 0, k] for k in range(levels)])
        cot = join_levels([recv_rows[e, 1, k] for k in range(levels)])
        back, rest = column_work(
            state, cot, syn_ref, ana_ref, gain_ref, w_in_ref, b_in_ref, w_mid_ref, b_mid_ref,
            w_out_ref,
        )
        half = back.shape[1] // levels
        for k in range(levels):
            back_rows[e, k] = jnp.concatenate(
                [back[p * waves : (p + 1) * waves, k * half : (k + 1) * half] for p in range(2)],
                axis=1,
            )

        @pl.when(e < members - 1)
        def _():
            start_back(e)

        normed, delta_one, act_one, delta_two, act_two, column_cot, gain_sum = rest
        first, second = w_in_ref.size // 128, w_mid_ref.size // 128
        add_blocks(grads_ref, 0, dot(normed, delta_one, TN))
        add_blocks(grads_ref, first, dot(act_one, delta_two, TN))
        add_blocks(grads_ref, first + second, dot(act_two, column_cot, TN))
        at = 0
        for value in (
            gain_sum,
            jnp.sum(delta_one.astype(jnp.float32), axis=0, keepdims=True),
            jnp.sum(delta_two.astype(jnp.float32), axis=0, keepdims=True),
        ):
            add_blocks(small_ref, at, value)
            at += value.shape[1] // 128
        return carry

    lax.fori_loop(0, members, member, 0)

    half_rows, few = their_half.shape[0], their_small.shape[0]
    pair = send(
        grads_ref.at[pl.ds((1 - core) * half_rows, half_rows)], their_half,
        pair_sems.at[0], pair_sems.at[1], partner,
    )
    small_pair = send(
        small_ref.at[pl.ds((1 - core) * few, few)], their_small,
        small_pair_sems.at[0], small_pair_sems.at[1], partner,
    )
    pair.wait()
    small_pair.wait()
    mine = grads_ref[pl.ds(pl.multiple_of(core * half_rows, half_rows), half_rows)]
    rs_src[...] = (mine + their_half[...]).astype(rs_src.dtype).reshape(rs_src.shape)
    mine = small_ref[pl.ds(pl.multiple_of(core * few, few), few)]
    small_src[...] = (mine + their_small[...]).astype(small_src.dtype)

    def visit_rs(lat, low):
        peer = (lat, low + core)
        send(
            rs_src.at[lat * 2 + low // 2], rs_recv.at[chip], rs_sems.at[0], rs_sems.at[1], peer
        )
        send(small_src, small_recv.at[chip], small_sems.at[0], small_sems.at[1], peer)

    each_chip(i, j, visit_rs)
    start_back(members - 1)

    rs_recv[chip] = rs_src[chip]
    small_recv[chip] = small_src[...]
    await_bytes(rs_src.at[pl.ds(0, chips - 1)], rs_sems.at[1])
    summed = jnp.sum(rs_recv[...].astype(jnp.float32), axis=0).astype(ag_src.dtype)
    ag_src[...] = summed
    total_ref[core, chip] = summed

    def visit_ag(lat, low):
        send(
            ag_src, total_ref.at[core, chip], ag_sems.at[0], ag_sems.at[1], (lat, low + core)
        )

    each_chip(i, j, visit_ag)
    await_bytes(small_recv.at[pl.ds(0, chips - 1)], small_sems.at[1])
    small_total[core] = jnp.sum(small_recv[...].astype(jnp.float32), axis=0)
    small_swap = send(
        small_total.at[core], small_total.at[core],
        small_swap_sems.at[0], small_swap_sems.at[1], partner,
    )
    await_bytes(rs_src.at[pl.ds(0, chips - 1)], ag_sems.at[1])
    swap = send(
        total_ref.at[core], total_ref.at[core], swap_sems.at[0], swap_sems.at[1], partner
    )
    many = rs_src.at[pl.ds(0, chips - 1)]
    await_bytes(many, rs_sems.at[0])
    await_bytes(many, ag_sems.at[0])
    await_bytes(small_recv.at[pl.ds(0, chips - 1)], small_sems.at[0])
    await_bytes(landed_ref.at[:, :, 0], local_sems.at[0])
    many = landed_ref.at[:, :, pl.ds(0, n - 1)]
    await_bytes(many, back_sems.at[0])
    await_bytes(many, back_sems.at[1])
    await_bytes(four_ref.at[:, :, :, pl.ds(0, n - 1)], out_sems.at[0])
    small_swap.wait()
    factor = float(MEMBERS * NLAT * NLON) ** (-0.5)
    at = 0
    for ref in (g_gain_ref, g_b_in_ref, g_b_mid_ref):
        for b in range(ref.shape[1] // 128):
            row = small_total[at // few, pl.ds(at % few, 1)]
            ref[:, b * 128 : (b + 1) * 128] = row * factor
            at += 1
    swap.wait()
    at, each = 0, total_ref.shape[2]
    for ref in (g_in_ref, g_mid_ref, g_out_ref):
        rows = ref.shape[0]
        for b in range(ref.shape[1] // 128):
            part = total_ref[at // half_rows, pl.ds(at % half_rows // each, rows // each)]
            ref[:, b * 128 : (b + 1) * 128] = part.reshape(rows, 128)
            at += rows


def whole_step_call(four, waves_all, gain, w_in, b_in, w_mid, b_mid, w_out, n_lat, n_lev):
    members, kinds, slots, n, two, lanes = four.shape
    bf16, f32 = jnp.bfloat16, jnp.float32
    waves, longitudes = 2 * waves_all.shape[0], NLON
    params = (waves_all[None], gain[None], w_in, b_in[None], w_mid, b_mid[None], w_out)
    chips = n // 2
    grad_rows = (w_in.size + w_mid.size + w_out.size) // lanes
    half = grad_rows // 2
    slices = (chips, half // chips, lanes)
    few = 8
    small = (2 * few, lanes)
    dma = pltpu.SemaphoreType.DMA
    row = lambda a: jax.ShapeDtypeStruct((1, a.size), f32)
    out_shape = (
        jax.ShapeDtypeStruct((members, slots, n, two, lanes), bf16),
        jax.ShapeDtypeStruct(w_in.shape, bf16),
        jax.ShapeDtypeStruct(w_mid.shape, bf16),
        jax.ShapeDtypeStruct(w_out.shape, bf16),
        row(gain),
        row(b_in),
        row(b_mid),
    )
    return pl.pallas_call(
        functools.partial(whole_step, n),
        out_shape=out_shape,
        in_specs=[pl.BlockSpec(memory_space=pl.ANY)]
        + [pl.BlockSpec(memory_space=pltpu.VMEM)] * len(params),
        out_specs=[pl.BlockSpec(memory_space=pl.ANY)]
        + [pl.BlockSpec(memory_space=pltpu.VMEM)] * (len(out_shape) - 1),
        scratch_shapes=[
            pltpu.VMEM((members, kinds, n_lev, n_lat * slots, two, lanes), bf16),
            pltpu.VMEM((members, n_lev, n_lat * slots, two, lanes), bf16),
            pltpu.VMEM((2 * longitudes, 2 * waves), bf16),
            pltpu.VMEM((2 * waves, 2 * longitudes), bf16),
            pltpu.VMEM((grad_rows, lanes), f32),
            pltpu.VMEM(small, f32),
            pltpu.VMEM((half, lanes), f32),
            pltpu.VMEM((few, lanes), f32),
            pltpu.VMEM(slices, bf16),
            pltpu.VMEM(slices, bf16),
            pltpu.VMEM(slices[1:], bf16),
            pltpu.VMEM((2,) + slices, bf16),
            pltpu.VMEM((few, lanes), bf16),
            pltpu.VMEM((chips, few, lanes), bf16),
            pltpu.VMEM((2, few, lanes), f32),
            dma((1,)),
            dma((members,)),
            dma((members,)),
        ]
        + [dma((2,))] * 8
        + [dma((1,))],
        compiler_params=pltpu.CompilerParams(
            has_side_effects=True, vmem_limit_bytes=60 * 1024 * 1024
        ),
        name="whole_step",
    )(four, *params)


def local(
    n_lat, n_lev, spec_in, cotangent, legendre, quad_weights, wave_order, norm_gain, weight_in,
    bias_in, weight_mid, bias_mid, weight_out,
):
    bf16 = jnp.bfloat16
    n = n_lat * n_lev
    slots_here, degrees, members, lanes = spec_in.shape
    rows = NLAT // n
    own_waves = lax.dynamic_slice_in_dim(wave_order, lax.axis_index("lat") * slots_here, slots_here)
    living, shrink = spectral_masks(own_waves, degrees)
    basis_rows = jnp.where(living[:, :, None], legendre, jnp.zeros_like(legendre))
    lane = np.arange(lanes)
    apart = np.zeros((lanes, lanes), np.float32)
    apart[lane, (lane % 2) * (lanes // 2) + lane // 2] = 1.0
    apart = jnp.asarray(apart, bf16)

    pushed = (time_step * cotangent.astype(jnp.float32) * shrink[:, :, None, None]).astype(bf16)
    both = jnp.stack([spec_in, pushed], axis=3)
    both = jnp.einsum("slehk,kq->slehq", both, apart, preferred_element_type=jnp.float32)
    fourier = jnp.einsum(
        "slt,slehq->sehtq", basis_rows, both.astype(bf16), preferred_element_type=jnp.float32
    )
    weights = jnp.stack([jnp.ones_like(quad_weights), quad_weights])
    fourier = (fourier * weights[None, None, :, :, None]).astype(bf16)
    fourier = fourier.transpose(1, 2, 0, 3, 4)
    fourier = fourier.reshape(members, 2, slots_here, n, rows, lanes)
    landed, g_in, g_mid, g_out, g_gain, g_b_in, g_b_mid = whole_step_call(
        fourier, wave_order, norm_gain, weight_in, bias_in, weight_mid, bias_mid, weight_out,
        n_lat, n_lev,
    )
    landed = landed.reshape(members, slots_here, n * rows, lanes)
    landed = jnp.einsum(
        "estq,kq->setk", landed, apart, preferred_element_type=jnp.float32
    ).astype(bf16)
    grad_spec = cotangent.astype(jnp.float32) * shrink[:, :, None, None] + jnp.einsum(
        "slt,setk->slek", basis_rows, landed, preferred_element_type=jnp.float32
    )
    factor = float(MEMBERS * NLAT * NLON) ** (-0.5)
    g_in, g_mid, g_out = (g.astype(jnp.float32) * factor for g in (g_in, g_mid, g_out))
    return (grad_spec, g_gain[0], g_in, g_b_in[0], g_mid, g_b_mid[0], g_out)


def solution(mesh):
    split = P("lat", None, None, "lev")
    placed = (split, split, P("lat", None, None)) + (P(),) * 8
    return jax.shard_map(
        functools.partial(local, mesh.shape["lat"], mesh.shape["lev"]),
        mesh=mesh,
        in_specs=placed,
        out_specs=(split,) + (P(),) * 6,
        check_vma=False,
    )
```

```python
import functools
import math

import jax
import jax.numpy as jnp
import numpy as np
from jax import lax
from jax.experimental import pallas as pl
from jax.experimental.pallas import tpu as pltpu
from jax.sharding import PartitionSpec as P

WAVES = 171
NLAT = 256
NLON = 512
MEMBERS = 4

time_step = 0.5
norm_eps = 1e-06
MESH = pl.DeviceIdType.MESH


def spectral_masks(waves_held, degree_count):
    degree = jnp.arange(degree_count, dtype=jnp.int32)
    living = (waves_held[:, None] <= degree[None, :]) & (waves_held[:, None] < WAVES)
    ratio = (degree * (degree + 1)).astype(jnp.float32) / float(WAVES * (WAVES - 1))
    factor = 1.0 / (1.0 + ratio * ratio)
    shrink = jnp.where(living, factor[None, :], jnp.zeros_like(factor)[None, :])
    return (living, shrink)


def fourier_table(waves_all):
    shape = (NLON, waves_all.shape[1])
    longitude = lax.broadcasted_iota(jnp.int32, shape, 0)
    phase_steps = jnp.bitwise_and(waves_all * longitude, NLON - 1)
    angles = phase_steps.astype(jnp.float32) * (2.0 * math.pi / NLON)
    scale = jnp.where(waves_all < WAVES, math.sqrt(2.0 / NLON), 0.0).astype(jnp.float32)
    return jnp.concatenate(
        [jnp.cos(angles) * scale, -jnp.sin(angles) * scale], axis=1
    ).astype(jnp.bfloat16)


AROUND = (
    (1, 2), (2, 1), (0, 3), (3, 0), (1, 1), (2, 3), (0, 1), (3, 2), (1, 0), (2, 2), (0, 2),
    (3, 1), (2, 0), (1, 3), (3, 3),
)


def each_chip(i, j, visit):
    z = [lax.rem(i // 8 + d, 4) * 8 for d in range(4)]
    y = [lax.rem(lax.rem(i // 2, 4) + d, 4) * 2 for d in range(4)]
    x = lax.rem(i, 2) * 2 + j // 2

    def along_x(d):
        to = lax.rem(x + d, 4)
        return to // 2, lax.rem(to, 2) * 2

    for d in (1, 2, 3):
        high, low = along_x(d)
        visit(z[0] + y[0] + high, low)

    def turn(a, carry):
        across = [along_x(a + d) for d in range(4)]
        for at, (dz, dy) in enumerate(AROUND):
            high, low = across[at % 4]
            visit(z[dz] + y[dy] + high, low)
        return carry

    lax.fori_loop(0, 4, turn, 0)


def each_peer(i, j, visit):
    visit(i, j + 1 - 2 * lax.rem(j, 2))

    def both(lat, low):
        visit(lat, low)
        visit(lat, low + 1)

    each_chip(i, j, both)


def send(src, dst, send_sem, recv_sem, peer):
    copy = pltpu.make_async_remote_copy(
        src_ref=src, dst_ref=dst, send_sem=send_sem, recv_sem=recv_sem,
        device_id=peer, device_id_type=MESH,
    )
    copy.start()
    return copy


def await_bytes(like, sem):
    pltpu.make_async_copy(like, like, sem).wait()


def dot(a, b, dims):
    return lax.dot_general(a, b, (dims, ((), ())), preferred_element_type=jnp.float32)


def sigmoid(z):
    return 0.5 * jnp.tanh(0.5 * z) + 0.5


def join_levels(parts):
    half = parts[0].shape[1] // 2
    rows = []
    for p in range(2):
        rows.append(
            jnp.concatenate([a[:, p * half : (p + 1) * half] for a in parts], axis=1)
        )
    return jnp.concatenate(rows, axis=0)


def one_of_two(shape, long_dim, which):
    long = lax.broadcasted_iota(jnp.int32, shape, long_dim)
    short = lax.broadcasted_iota(jnp.int32, shape, 1 - long_dim)
    return jnp.where(long == 2 * short + which, 1.0, 0.0).astype(jnp.bfloat16)


NN, NT, TN = (((1,), (0,)), ((1,), (1,)), ((0,), (0,)))


def add_blocks(ref, start, value):
    rows, lanes = value.shape[0], ref.shape[1]
    for b in range(value.shape[1] // lanes):
        ref[pl.ds(start + b * rows, rows)] += value[:, b * lanes : (b + 1) * lanes]


def column_work(
    state, cot, syn_ref, ana_ref, gain_ref, w_in_ref, b_in_ref, w_mid_ref, b_mid_ref, w_out_ref
):
    bf16 = jnp.bfloat16
    columns = dot(syn_ref[...], state, NN).astype(bf16)
    column_cot = dot(syn_ref[...], cot, NN).astype(bf16)
    gain = gain_ref[...]
    inputs = columns.astype(jnp.float32)
    inverse = lax.rsqrt(jnp.mean(inputs * inputs, axis=1, keepdims=True) + norm_eps)
    normed = (inputs * inverse * gain).astype(bf16)
    pre_one = dot(normed, w_in_ref[...], NN) + b_in_ref[...]
    sig_one = sigmoid(pre_one)
    act_one = (pre_one * sig_one).astype(bf16)
    slope_one = sig_one * (1.0 + pre_one * (1.0 - sig_one))
    pre_two = dot(act_one, w_mid_ref[...], NN) + b_mid_ref[...]
    sig_two = sigmoid(pre_two)
    act_two = (pre_two * sig_two).astype(bf16)
    slope_two = sig_two * (1.0 + pre_two * (1.0 - sig_two))
    back_two = dot(column_cot, w_out_ref[...], NT)
    delta_two = (back_two * slope_two).astype(bf16)
    back_one = dot(delta_two, w_mid_ref[...], NT)
    delta_one = (back_one * slope_one).astype(bf16)
    back_norm = dot(delta_one, w_in_ref[...], NT)
    scaled = back_norm * gain
    grad_columns = inverse * scaled - inputs * (inverse * inverse * inverse) * jnp.mean(
        scaled * inputs, axis=1, keepdims=True
    )
    back = dot(ana_ref[...], grad_columns.astype(bf16), NN).astype(bf16)
    gain_sum = jnp.sum(back_norm * inputs * inverse, axis=0, keepdims=True)
    return back, (normed, delta_one, act_one, delta_two, act_two, column_cot, gain_sum)


def legendre_out(
    first_slot, orders_ref, quad_ref, spec_ref, cotangent_ref, legendre_ref, four_ref
):
    bf16, f32 = jnp.bfloat16, jnp.float32
    slots, degrees, members, lanes = spec_ref.shape
    pad = -(-degrees // 16) * 16
    rows = degrees * members
    spec_rows = spec_ref.reshape(slots, rows, lanes)
    cotangent_rows = cotangent_ref.reshape(slots, rows, lanes)
    four_rows = four_ref.reshape(members, 2, slots, NLAT, lanes)
    a = lax.broadcasted_iota(jnp.int32, (lanes, lanes), 0)
    b = lax.broadcasted_iota(jnp.int32, (lanes, lanes), 1)
    apart = jnp.where(
        a == jnp.where(b < lanes // 2, 2 * b, 2 * b - lanes + 1), 1.0, 0.0
    ).astype(bf16)
    degree = lax.broadcasted_iota(jnp.int32, (pad, rows), 0)
    row = lax.broadcasted_iota(jnp.int32, (pad, rows), 1)
    pick = jnp.concatenate(
        [jnp.where(row == members * degree + e, 1.0, 0.0).astype(bf16) for e in range(members)],
        axis=0,
    )
    quad = jnp.broadcast_to(quad_ref[...], (lanes, NLAT)).T

    def slot(s, carry):
        order = orders_ref[first_slot + s]
        degree = lax.shift_right_logical(lax.broadcasted_iota(jnp.int32, (rows, lanes), 0), 2)
        ratio = (degree * (degree + 1)).astype(f32) / float(WAVES * (WAVES - 1))
        living = jnp.logical_and(degree >= order, order < WAVES)
        shrink = jnp.where(living, 1.0 / (1.0 + ratio * ratio), 0.0)
        pushed = (time_step * cotangent_rows[s].astype(f32) * shrink).astype(bf16)
        both = jnp.concatenate(
            [dot(spec_rows[s], apart, NN).astype(bf16), dot(pushed, apart, NN).astype(bf16)],
            axis=1,
        )
        both = dot(pick, both, NN).astype(bf16)
        basis = legendre_ref[s].astype(f32)
        degree = lax.broadcasted_iota(jnp.int32, basis.shape, 0)
        living = jnp.logical_and(degree >= order, order < WAVES)
        basis = jnp.where(living, basis, 0.0).astype(bf16)
        for e in range(members):
            values = dot(basis, both[e * pad : e * pad + degrees], TN)
            four_rows[e, 0, s] = values[:, :lanes].astype(bf16)
            four_rows[e, 1, s] = (values[:, lanes:] * quad).astype(bf16)
        return carry

    lax.fori_loop(0, slots, slot, 0)


def whole_step(
    n, orders_ref, quad_ref, spec_ref, cotangent_ref, legendre_ref, waves_ref, gain_ref, w_in_ref, b_in_ref, w_mid_ref, b_mid_ref,
    w_out_ref, landed_ref, g_in_ref, g_mid_ref, g_out_ref, g_gain_ref, g_b_in_ref, g_b_mid_ref,
    four_ref, recv_ref, back_ref, syn_ref, ana_ref, grads_ref, small_ref,
    their_half, their_small, rs_src, rs_recv, ag_src, total_ref, small_src, small_recv,
    small_total, out_sems, arrive_sems, pair_sems, back_sems, rs_sems, ag_sems,
    swap_sems, small_sems, small_pair_sems, small_swap_sems, local_sems,
):
    i, j = lax.axis_index("lat"), lax.axis_index("lev")
    me = i * 4 + j
    core = lax.rem(j, 2)
    chip = i * 2 + j // 2
    chips = n // 2
    partner = (i, j + 1 - 2 * core)
    members, slots = landed_ref.shape[:2]
    levels = recv_ref.shape[2]
    waves, longitudes = 2 * waves_ref.shape[1], NLON

    def arriving(e):
        return recv_ref.at[e, :, j, pl.ds(i * slots, slots)]

    def start_out(e):
        def visit(lat, lev):
            send(
                four_ref.at[e, :, :, lat * 4 + lev], arriving(e),
                out_sems.at[0], arrive_sems.at[e], (lat, lev),
            )

        each_peer(i, j, visit)
        recv_ref[e, :, j, pl.ds(i * slots, slots)] = four_ref[e, :, :, me]

    barrier = pltpu.get_barrier_semaphore()

    def greet(lat, lev):
        pl.semaphore_signal(barrier, inc=1, device_id=(lat, lev), device_id_type=MESH)

    each_peer(i, j, greet)
    legendre_out(i * slots, orders_ref, quad_ref, spec_ref, cotangent_ref, legendre_ref, four_ref)
    pl.semaphore_wait(barrier, n - 1)
    start_out(0)
    start_out(1)
    grads_ref[...] = jnp.zeros_like(grads_ref)
    small_ref[...] = jnp.zeros_like(small_ref)
    table = fourier_table(waves_ref[...])
    for r in range(2):
        span = pl.ds(r * longitudes, longitudes)
        syn_ref[span] = dot(table, one_of_two((waves, 2 * waves), 1, r), NN).astype(jnp.bfloat16)
        ana_ref[:, span] = dot(one_of_two((2 * waves, waves), 0, r), table, NT).astype(
            jnp.bfloat16
        )

    def start_back(e):
        def visit(lat, lev):
            send(
                back_ref.at[e, lev, pl.ds(lat * slots, slots)], landed_ref.at[e, :, me],
                back_sems.at[0], back_sems.at[1], (lat, lev),
            )

        pltpu.make_async_copy(
            back_ref.at[e, j, pl.ds(i * slots, slots)], landed_ref.at[e, :, me],
            local_sems.at[0],
        ).start()
        each_peer(i, j, visit)

    recv_rows = recv_ref.reshape(members, 2, levels, 2 * n // 4 * slots, recv_ref.shape[-1])
    back_rows = back_ref.reshape(members, levels, 2 * n // 4 * slots, back_ref.shape[-1])

    def member(e, carry):
        @pl.when(e < members - 2)
        def _():
            start_out(e + 2)

        await_bytes(four_ref.at[e, :, :, pl.ds(0, n - 1)], arrive_sems.at[e])
        state = join_levels([recv_rows[e, 0, k] for k in range(levels)])
        cot = join_levels([recv_rows[e, 1, k] for k in range(levels)])
        back, rest = column_work(
            state, cot, syn_ref, ana_ref, gain_ref, w_in_ref, b_in_ref, w_mid_ref, b_mid_ref,
            w_out_ref,
        )
        half = back.shape[1] // levels
        for k in range(levels):
            back_rows[e, k] = jnp.concatenate(
                [back[p * waves : (p + 1) * waves, k * half : (k + 1) * half] for p in range(2)],
                axis=1,
            )

        @pl.when(e < members - 1)
        def _():
            start_back(e)

        normed, delta_one, act_one, delta_two, act_two, column_cot, gain_sum = rest
        first, second = w_in_ref.size // 128, w_mid_ref.size // 128
        add_blocks(grads_ref, 0, dot(normed, delta_one, TN))
        add_blocks(grads_ref, first, dot(act_one, delta_two, TN))
        add_blocks(grads_ref, first + second, dot(act_two, column_cot, TN))
        at = 0
        for value in (
            gain_sum,
            jnp.sum(delta_one.astype(jnp.float32), axis=0, keepdims=True),
            jnp.sum(delta_two.astype(jnp.float32), axis=0, keepdims=True),
        ):
            add_blocks(small_ref, at, value)
            at += value.shape[1] // 128
        return carry

    lax.fori_loop(0, members, member, 0)

    half_rows, few = their_half.shape[0], their_small.shape[0]
    pair = send(
        grads_ref.at[pl.ds((1 - core) * half_rows, half_rows)], their_half,
        pair_sems.at[0], pair_sems.at[1], partner,
    )
    small_pair = send(
        small_ref.at[pl.ds((1 - core) * few, few)], their_small,
        small_pair_sems.at[0], small_pair_sems.at[1], partner,
    )
    pair.wait()
    small_pair.wait()
    mine = grads_ref[pl.ds(pl.multiple_of(core * half_rows, half_rows), half_rows)]
    rs_src[...] = (mine + their_half[...]).astype(rs_src.dtype).reshape(rs_src.shape)
    mine = small_ref[pl.ds(pl.multiple_of(core * few, few), few)]
    small_src[...] = (mine + their_small[...]).astype(small_src.dtype)

    def visit_rs(lat, low):
        peer = (lat, low + core)
        send(
            rs_src.at[lat * 2 + low // 2], rs_recv.at[chip], rs_sems.at[0], rs_sems.at[1], peer
        )
        send(small_src, small_recv.at[chip], small_sems.at[0], small_sems.at[1], peer)

    each_chip(i, j, visit_rs)
    start_back(members - 1)

    rs_recv[chip] = rs_src[chip]
    small_recv[chip] = small_src[...]
    await_bytes(rs_src.at[pl.ds(0, chips - 1)], rs_sems.at[1])
    summed = jnp.sum(rs_recv[...].astype(jnp.float32), axis=0).astype(ag_src.dtype)
    ag_src[...] = summed
    total_ref[core, chip] = summed

    def visit_ag(lat, low):
        send(
            ag_src, total_ref.at[core, chip], ag_sems.at[0], ag_sems.at[1], (lat, low + core)
        )

    each_chip(i, j, visit_ag)
    await_bytes(small_recv.at[pl.ds(0, chips - 1)], small_sems.at[1])
    small_total[core] = jnp.sum(small_recv[...].astype(jnp.float32), axis=0)
    small_swap = send(
        small_total.at[core], small_total.at[core],
        small_swap_sems.at[0], small_swap_sems.at[1], partner,
    )
    await_bytes(rs_src.at[pl.ds(0, chips - 1)], ag_sems.at[1])
    swap = send(
        total_ref.at[core], total_ref.at[core], swap_sems.at[0], swap_sems.at[1], partner
    )
    many = rs_src.at[pl.ds(0, chips - 1)]
    await_bytes(many, rs_sems.at[0])
    await_bytes(many, ag_sems.at[0])
    await_bytes(small_recv.at[pl.ds(0, chips - 1)], small_sems.at[0])
    await_bytes(landed_ref.at[:, :, 0], local_sems.at[0])
    many = landed_ref.at[:, :, pl.ds(0, n - 1)]
    await_bytes(many, back_sems.at[0])
    await_bytes(many, back_sems.at[1])
    await_bytes(four_ref.at[:, :, :, pl.ds(0, n - 1)], out_sems.at[0])
    small_swap.wait()
    factor = float(MEMBERS * NLAT * NLON) ** (-0.5)
    at = 0
    for ref in (g_gain_ref, g_b_in_ref, g_b_mid_ref):
        for b in range(ref.shape[1] // 128):
            row = small_total[at // few, pl.ds(at % few, 1)]
            ref[:, b * 128 : (b + 1) * 128] = row * factor
            at += 1
    swap.wait()
    at, each = 0, total_ref.shape[2]
    for ref in (g_in_ref, g_mid_ref, g_out_ref):
        rows = ref.shape[0]
        for b in range(ref.shape[1] // 128):
            part = total_ref[at // half_rows, pl.ds(at % half_rows // each, rows // each)]
            ref[:, b * 128 : (b + 1) * 128] = part.reshape(rows, 128)
            at += rows


def whole_step_call(spec_in, cotangent, legendre, quad, waves_all, gain, w_in, b_in, w_mid, b_mid, w_out, n_lat, n_lev):
    slots, _, members, lanes = spec_in.shape
    kinds, n, two = 2, n_lat * n_lev, NLAT // (n_lat * n_lev)
    bf16, f32 = jnp.bfloat16, jnp.float32
    waves, longitudes = 2 * waves_all.shape[0], NLON
    params = (quad[None], spec_in, cotangent, legendre, waves_all[None], gain[None], w_in, b_in[None], w_mid, b_mid[None], w_out)
    chips = n // 2
    grad_rows = (w_in.size + w_mid.size + w_out.size) // lanes
    half = grad_rows // 2
    slices = (chips, half // chips, lanes)
    few = 8
    small = (2 * few, lanes)
    dma = pltpu.SemaphoreType.DMA
    row = lambda a: jax.ShapeDtypeStruct((1, a.size), f32)
    out_shape = (
        jax.ShapeDtypeStruct((members, slots, n, two, lanes), bf16),
        jax.ShapeDtypeStruct(w_in.shape, bf16),
        jax.ShapeDtypeStruct(w_mid.shape, bf16),
        jax.ShapeDtypeStruct(w_out.shape, bf16),
        row(gain),
        row(b_in),
        row(b_mid),
    )
    return pl.pallas_call(
        functools.partial(whole_step, n),
        out_shape=out_shape,
        in_specs=[pl.BlockSpec(memory_space=pltpu.SMEM)]
        + [pl.BlockSpec(memory_space=pltpu.VMEM)] * len(params),
        out_specs=[pl.BlockSpec(memory_space=pl.ANY)]
        + [pl.BlockSpec(memory_space=pltpu.VMEM)] * (len(out_shape) - 1),
        scratch_shapes=[
            pltpu.VMEM((members, kinds, slots, n, two, lanes), bf16),
            pltpu.VMEM((members, kinds, n_lev, n_lat * slots, two, lanes), bf16),
            pltpu.VMEM((members, n_lev, n_lat * slots, two, lanes), bf16),
            pltpu.VMEM((2 * longitudes, 2 * waves), bf16),
            pltpu.VMEM((2 * waves, 2 * longitudes), bf16),
            pltpu.VMEM((grad_rows, lanes), f32),
            pltpu.VMEM(small, f32),
            pltpu.VMEM((half, lanes), f32),
            pltpu.VMEM((few, lanes), f32),
            pltpu.VMEM(slices, bf16),
            pltpu.VMEM(slices, bf16),
            pltpu.VMEM(slices[1:], bf16),
            pltpu.VMEM((2,) + slices, bf16),
            pltpu.VMEM((few, lanes), bf16),
            pltpu.VMEM((chips, few, lanes), bf16),
            pltpu.VMEM((2, few, lanes), f32),
            dma((1,)),
            dma((members,)),
        ]
        + [dma((2,))] * 8
        + [dma((1,))],
        compiler_params=pltpu.CompilerParams(
            collective_id=0, has_side_effects=True, vmem_limit_bytes=60 * 1024 * 1024
        ),
        name="whole_step",
    )(waves_all, *params)


def local(
    n_lat, n_lev, spec_in, cotangent, legendre, quad_weights, wave_order, norm_gain, weight_in,
    bias_in, weight_mid, bias_mid, weight_out,
):
    bf16 = jnp.bfloat16
    n = n_lat * n_lev
    slots_here, degrees, members, lanes = spec_in.shape
    rows = NLAT // n
    own_waves = lax.dynamic_slice_in_dim(wave_order, lax.axis_index("lat") * slots_here, slots_here)
    living, shrink = spectral_masks(own_waves, degrees)
    basis_rows = jnp.where(living[:, :, None], legendre, jnp.zeros_like(legendre))
    lane = np.arange(lanes)
    apart = np.zeros((lanes, lanes), np.float32)
    apart[lane, (lane % 2) * (lanes // 2) + lane // 2] = 1.0
    apart = jnp.asarray(apart, bf16)

    landed, g_in, g_mid, g_out, g_gain, g_b_in, g_b_mid = whole_step_call(
        spec_in, cotangent, legendre, quad_weights, wave_order, norm_gain, weight_in, bias_in, weight_mid, bias_mid, weight_out,
        n_lat, n_lev,
    )
    landed = landed.reshape(members, slots_here, n * rows, lanes)
    landed = jnp.einsum(
        "estq,kq->setk", landed, apart, preferred_element_type=jnp.float32
    ).astype(bf16)
    grad_spec = cotangent.astype(jnp.float32) * shrink[:, :, None, None] + jnp.einsum(
        "slt,setk->slek", basis_rows, landed, preferred_element_type=jnp.float32
    )
    factor = float(MEMBERS * NLAT * NLON) ** (-0.5)
    g_in, g_mid, g_out = (g.astype(jnp.float32) * factor for g in (g_in, g_mid, g_out))
    return (grad_spec, g_gain[0], g_in, g_b_in[0], g_mid, g_b_mid[0], g_out)


def solution(mesh):
    split = P("lat", None, None, "lev")
    placed = (split, split, P("lat", None, None)) + (P(),) * 8
    return jax.shard_map(
        functools.partial(local, mesh.shape["lat"], mesh.shape["lev"]),
        mesh=mesh,
        in_specs=placed,
        out_specs=(split,) + (P(),) * 6,
        check_vma=False,
    )
```

```python
import functools
import math

import jax
import jax.numpy as jnp
import numpy as np
from jax import lax
from jax.experimental import pallas as pl
from jax.experimental.pallas import tpu as pltpu
from jax.sharding import PartitionSpec as P

WAVES = 171
NLAT = 256
NLON = 512
MEMBERS = 4

time_step = 0.5
norm_eps = 1e-06
MESH = pl.DeviceIdType.MESH


def spectral_masks(waves_held, degree_count):
    degree = jnp.arange(degree_count, dtype=jnp.int32)
    living = (waves_held[:, None] <= degree[None, :]) & (waves_held[:, None] < WAVES)
    ratio = (degree * (degree + 1)).astype(jnp.float32) / float(WAVES * (WAVES - 1))
    factor = 1.0 / (1.0 + ratio * ratio)
    shrink = jnp.where(living, factor[None, :], jnp.zeros_like(factor)[None, :])
    return (living, shrink)


def fourier_table(waves_all):
    shape = (NLON, waves_all.shape[1])
    longitude = lax.broadcasted_iota(jnp.int32, shape, 0)
    phase_steps = jnp.bitwise_and(waves_all * longitude, NLON - 1)
    angles = phase_steps.astype(jnp.float32) * (2.0 * math.pi / NLON)
    scale = jnp.where(waves_all < WAVES, math.sqrt(2.0 / NLON), 0.0).astype(jnp.float32)
    return jnp.concatenate(
        [jnp.cos(angles) * scale, -jnp.sin(angles) * scale], axis=1
    ).astype(jnp.bfloat16)


AROUND = (
    (1, 2), (2, 1), (0, 3), (3, 0), (1, 1), (2, 3), (0, 1), (3, 2), (1, 0), (2, 2), (0, 2),
    (3, 1), (2, 0), (1, 3), (3, 3),
)


def each_chip(i, j, visit):
    z = [lax.rem(i // 8 + d, 4) * 8 for d in range(4)]
    y = [lax.rem(lax.rem(i // 2, 4) + d, 4) * 2 for d in range(4)]
    x = lax.rem(i, 2) * 2 + j // 2

    def along_x(d):
        to = lax.rem(x + d, 4)
        return to // 2, lax.rem(to, 2) * 2

    for d in (1, 2, 3):
        high, low = along_x(d)
        visit(z[0] + y[0] + high, low)

    def turn(a, carry):
        across = [along_x(a + d) for d in range(4)]
        for at, (dz, dy) in enumerate(AROUND):
            high, low = across[at % 4]
            visit(z[dz] + y[dy] + high, low)
        return carry

    lax.fori_loop(0, 4, turn, 0)


def each_peer(i, j, visit):
    visit(i, j + 1 - 2 * lax.rem(j, 2))

    def both(lat, low):
        visit(lat, low)
        visit(lat, low + 1)

    each_chip(i, j, both)


def send(src, dst, send_sem, recv_sem, peer):
    copy = pltpu.make_async_remote_copy(
        src_ref=src, dst_ref=dst, send_sem=send_sem, recv_sem=recv_sem,
        device_id=peer, device_id_type=MESH,
    )
    copy.start()
    return copy


def await_bytes(like, sem):
    pltpu.make_async_copy(like, like, sem).wait()


def dot(a, b, dims):
    return lax.dot_general(a, b, (dims, ((), ())), preferred_element_type=jnp.float32)


def sigmoid(z):
    return 0.5 * jnp.tanh(0.5 * z) + 0.5


def join_levels(parts):
    half = parts[0].shape[1] // 2
    rows = []
    for p in range(2):
        rows.append(
            jnp.concatenate([a[:, p * half : (p + 1) * half] for a in parts], axis=1)
        )
    return jnp.concatenate(rows, axis=0)


def one_of_two(shape, long_dim, which):
    long = lax.broadcasted_iota(jnp.int32, shape, long_dim)
    short = lax.broadcasted_iota(jnp.int32, shape, 1 - long_dim)
    return jnp.where(long == 2 * short + which, 1.0, 0.0).astype(jnp.bfloat16)


NN, NT, TN = (((1,), (0,)), ((1,), (1,)), ((0,), (0,)))


def add_blocks(ref, start, value):
    rows, lanes = value.shape[0], ref.shape[1]
    for b in range(value.shape[1] // lanes):
        ref[pl.ds(start + b * rows, rows)] += value[:, b * lanes : (b + 1) * lanes]


def column_work(
    state, cot, syn_ref, ana_ref, gain_ref, w_in_ref, b_in_ref, w_mid_ref, b_mid_ref, w_out_ref
):
    bf16 = jnp.bfloat16
    columns = dot(syn_ref[...], state, NN).astype(bf16)
    column_cot = dot(syn_ref[...], cot, NN).astype(bf16)
    gain = gain_ref[...]
    inputs = columns.astype(jnp.float32)
    inverse = lax.rsqrt(jnp.mean(inputs * inputs, axis=1, keepdims=True) + norm_eps)
    normed = (inputs * inverse * gain).astype(bf16)
    pre_one = dot(normed, w_in_ref[...], NN) + b_in_ref[...]
    sig_one = sigmoid(pre_one)
    act_one = (pre_one * sig_one).astype(bf16)
    slope_one = sig_one * (1.0 + pre_one * (1.0 - sig_one))
    pre_two = dot(act_one, w_mid_ref[...], NN) + b_mid_ref[...]
    sig_two = sigmoid(pre_two)
    act_two = (pre_two * sig_two).astype(bf16)
    slope_two = sig_two * (1.0 + pre_two * (1.0 - sig_two))
    back_two = dot(column_cot, w_out_ref[...], NT)
    delta_two = (back_two * slope_two).astype(bf16)
    back_one = dot(delta_two, w_mid_ref[...], NT)
    delta_one = (back_one * slope_one).astype(bf16)
    back_norm = dot(delta_one, w_in_ref[...], NT)
    scaled = back_norm * gain
    grad_columns = inverse * scaled - inputs * (inverse * inverse * inverse) * jnp.mean(
        scaled * inputs, axis=1, keepdims=True
    )
    back = dot(ana_ref[...], grad_columns.astype(bf16), NN).astype(bf16)
    gain_sum = jnp.sum(back_norm * inputs * inverse, axis=0, keepdims=True)
    return back, (normed, delta_one, act_one, delta_two, act_two, column_cot, gain_sum)


def legendre_out(
    first_slot, orders_ref, quad_ref, spec_ref, cotangent_ref, legendre_ref, four_ref
):
    bf16, f32 = jnp.bfloat16, jnp.float32
    slots, degrees, members, lanes = spec_ref.shape
    pad = -(-degrees // 16) * 16
    rows = degrees * members
    spec_rows = spec_ref.reshape(slots, rows, lanes)
    cotangent_rows = cotangent_ref.reshape(slots, rows, lanes)
    four_rows = four_ref.reshape(members, 2, slots, NLAT, lanes)
    a = lax.broadcasted_iota(jnp.int32, (lanes, lanes), 0)
    b = lax.broadcasted_iota(jnp.int32, (lanes, lanes), 1)
    apart = jnp.where(
        a == jnp.where(b < lanes // 2, 2 * b, 2 * b - lanes + 1), 1.0, 0.0
    ).astype(bf16)
    degree = lax.broadcasted_iota(jnp.int32, (pad, rows), 0)
    row = lax.broadcasted_iota(jnp.int32, (pad, rows), 1)
    pick = jnp.concatenate(
        [jnp.where(row == members * degree + e, 1.0, 0.0).astype(bf16) for e in range(members)],
        axis=0,
    )
    quad = jnp.broadcast_to(quad_ref[...], (lanes, NLAT)).T

    def slot(s, carry):
        order = orders_ref[first_slot + s]
        degree = lax.shift_right_logical(lax.broadcasted_iota(jnp.int32, (rows, lanes), 0), 2)
        ratio = (degree * (degree + 1)).astype(f32) / float(WAVES * (WAVES - 1))
        living = jnp.logical_and(degree >= order, order < WAVES)
        shrink = jnp.where(living, 1.0 / (1.0 + ratio * ratio), 0.0)
        pushed = (time_step * cotangent_rows[s].astype(f32) * shrink).astype(bf16)
        both = jnp.concatenate(
            [dot(spec_rows[s], apart, NN).astype(bf16), dot(pushed, apart, NN).astype(bf16)],
            axis=1,
        )
        both = dot(pick, both, NN).astype(bf16)
        basis = legendre_ref[s].astype(f32)
        degree = lax.broadcasted_iota(jnp.int32, basis.shape, 0)
        living = jnp.logical_and(degree >= order, order < WAVES)
        basis = jnp.where(living, basis, 0.0).astype(bf16)
        for e in range(members):
            values = dot(basis, both[e * pad : e * pad + degrees], TN)
            four_rows[e, 0, s] = values[:, :lanes].astype(bf16)
            four_rows[e, 1, s] = (values[:, lanes:] * quad).astype(bf16)
        return carry

    lax.fori_loop(0, slots, slot, 0)


def whole_step(
    n, orders_ref, quad_ref, spec_ref, cotangent_ref, legendre_ref, waves_ref, gain_ref, w_in_ref, b_in_ref, w_mid_ref, b_mid_ref,
    w_out_ref, landed_ref, g_in_ref, g_mid_ref, g_out_ref, g_gain_ref, g_b_in_ref, g_b_mid_ref,
    four_ref, recv_ref, back_ref, syn_ref, ana_ref, grads_ref, small_ref,
    their_half, their_small, rs_src, rs_recv, ag_src, total_ref, small_src, small_recv,
    small_total, out_sems, arrive_sems, pair_sems, back_sems, rs_sems, ag_sems,
    swap_sems, small_sems, small_pair_sems, small_swap_sems, local_sems,
):
    i, j = lax.axis_index("lat"), lax.axis_index("lev")
    me = i * 4 + j
    core = lax.rem(j, 2)
    chip = i * 2 + j // 2
    chips = n // 2
    partner = (i, j + 1 - 2 * core)
    members, slots = landed_ref.shape[:2]
    levels = recv_ref.shape[2]
    waves, longitudes = 2 * waves_ref.shape[1], NLON

    def arriving(e):
        return recv_ref.at[e, :, j, pl.ds(i * slots, slots)]

    def start_out(e):
        def visit(lat, lev):
            send(
                four_ref.at[e, :, :, lat * 4 + lev], arriving(e),
                out_sems.at[0], arrive_sems.at[e], (lat, lev),
            )

        each_peer(i, j, visit)
        recv_ref[e, :, j, pl.ds(i * slots, slots)] = four_ref[e, :, :, me]

    barrier = pltpu.get_barrier_semaphore()

    def greet(lat, lev):
        pl.semaphore_signal(barrier, inc=1, device_id=(lat, lev), device_id_type=MESH)

    each_peer(i, j, greet)
    legendre_out(i * slots, orders_ref, quad_ref, spec_ref, cotangent_ref, legendre_ref, four_ref)
    pl.semaphore_wait(barrier, n - 1)
    start_out(0)
    start_out(1)
    grads_ref[...] = jnp.zeros_like(grads_ref)
    small_ref[...] = jnp.zeros_like(small_ref)
    table = fourier_table(waves_ref[...])
    for r in range(2):
        span = pl.ds(r * longitudes, longitudes)
        syn_ref[span] = dot(table, one_of_two((waves, 2 * waves), 1, r), NN).astype(jnp.bfloat16)
        ana_ref[:, span] = dot(one_of_two((2 * waves, waves), 0, r), table, NT).astype(
            jnp.bfloat16
        )

    def start_back(e):
        def visit(lat, lev):
            send(
                back_ref.at[e, lev, pl.ds(lat * slots, slots)], landed_ref.at[e, :, me],
                back_sems.at[0], back_sems.at[1], (lat, lev),
            )

        pltpu.make_async_copy(
            back_ref.at[e, j, pl.ds(i * slots, slots)], landed_ref.at[e, :, me],
            local_sems.at[0],
        ).start()
        each_peer(i, j, visit)

    recv_rows = recv_ref.reshape(members, 2, levels, 2 * n // 4 * slots, recv_ref.shape[-1])
    back_rows = back_ref.reshape(members, levels, 2 * n // 4 * slots, back_ref.shape[-1])

    def member(e, carry):
        @pl.when(e < members - 2)
        def _():
            start_out(e + 2)

        await_bytes(four_ref.at[e, :, :, pl.ds(0, n - 1)], arrive_sems.at[e])

        @pl.when(e == members - 1)
        def _():
            for early in range(members - 1):
                start_back(early)

        state = join_levels([recv_rows[e, 0, k] for k in range(levels)])
        cot = join_levels([recv_rows[e, 1, k] for k in range(levels)])
        back, rest = column_work(
            state, cot, syn_ref, ana_ref, gain_ref, w_in_ref, b_in_ref, w_mid_ref, b_mid_ref,
            w_out_ref,
        )
        half = back.shape[1] // levels
        for k in range(levels):
            back_rows[e, k] = jnp.concatenate(
                [back[p * waves : (p + 1) * waves, k * half : (k + 1) * half] for p in range(2)],
                axis=1,
            )

        normed, delta_one, act_one, delta_two, act_two, column_cot, gain_sum = rest
        first, second = w_in_ref.size // 128, w_mid_ref.size // 128
        add_blocks(grads_ref, 0, dot(normed, delta_one, TN))
        add_blocks(grads_ref, first, dot(act_one, delta_two, TN))
        add_blocks(grads_ref, first + second, dot(act_two, column_cot, TN))
        at = 0
        for value in (
            gain_sum,
            jnp.sum(delta_one.astype(jnp.float32), axis=0, keepdims=True),
            jnp.sum(delta_two.astype(jnp.float32), axis=0, keepdims=True),
        ):
            add_blocks(small_ref, at, value)
            at += value.shape[1] // 128
        return carry

    lax.fori_loop(0, members, member, 0)

    half_rows, few = their_half.shape[0], their_small.shape[0]
    pair = send(
        grads_ref.at[pl.ds((1 - core) * half_rows, half_rows)], their_half,
        pair_sems.at[0], pair_sems.at[1], partner,
    )
    small_pair = send(
        small_ref.at[pl.ds((1 - core) * few, few)], their_small,
        small_pair_sems.at[0], small_pair_sems.at[1], partner,
    )
    pair.wait()
    small_pair.wait()
    mine = grads_ref[pl.ds(pl.multiple_of(core * half_rows, half_rows), half_rows)]
    rs_src[...] = (mine + their_half[...]).astype(rs_src.dtype).reshape(rs_src.shape)
    mine = small_ref[pl.ds(pl.multiple_of(core * few, few), few)]
    small_src[...] = (mine + their_small[...]).astype(small_src.dtype)

    def visit_rs(lat, low):
        peer = (lat, low + core)
        send(
            rs_src.at[lat * 2 + low // 2], rs_recv.at[chip], rs_sems.at[0], rs_sems.at[1], peer
        )
        send(small_src, small_recv.at[chip], small_sems.at[0], small_sems.at[1], peer)

    each_chip(i, j, visit_rs)
    start_back(members - 1)

    rs_recv[chip] = rs_src[chip]
    small_recv[chip] = small_src[...]
    await_bytes(rs_src.at[pl.ds(0, chips - 1)], rs_sems.at[1])
    summed = jnp.sum(rs_recv[...].astype(jnp.float32), axis=0).astype(ag_src.dtype)
    ag_src[...] = summed
    total_ref[core, chip] = summed

    def visit_ag(lat, low):
        send(
            ag_src, total_ref.at[core, chip], ag_sems.at[0], ag_sems.at[1], (lat, low + core)
        )

    each_chip(i, j, visit_ag)
    await_bytes(small_recv.at[pl.ds(0, chips - 1)], small_sems.at[1])
    small_total[core] = jnp.sum(small_recv[...].astype(jnp.float32), axis=0)
    small_swap = send(
        small_total.at[core], small_total.at[core],
        small_swap_sems.at[0], small_swap_sems.at[1], partner,
    )
    await_bytes(rs_src.at[pl.ds(0, chips - 1)], ag_sems.at[1])
    swap = send(
        total_ref.at[core], total_ref.at[core], swap_sems.at[0], swap_sems.at[1], partner
    )
    many = rs_src.at[pl.ds(0, chips - 1)]
    await_bytes(many, rs_sems.at[0])
    await_bytes(many, ag_sems.at[0])
    await_bytes(small_recv.at[pl.ds(0, chips - 1)], small_sems.at[0])
    await_bytes(landed_ref.at[:, :, 0], local_sems.at[0])
    many = landed_ref.at[:, :, pl.ds(0, n - 1)]
    await_bytes(many, back_sems.at[0])
    await_bytes(many, back_sems.at[1])
    await_bytes(four_ref.at[:, :, :, pl.ds(0, n - 1)], out_sems.at[0])
    small_swap.wait()
    factor = float(MEMBERS * NLAT * NLON) ** (-0.5)
    at = 0
    for ref in (g_gain_ref, g_b_in_ref, g_b_mid_ref):
        for b in range(ref.shape[1] // 128):
            row = small_total[at // few, pl.ds(at % few, 1)]
            ref[:, b * 128 : (b + 1) * 128] = row * factor
            at += 1
    swap.wait()
    at, each = 0, total_ref.shape[2]
    for ref in (g_in_ref, g_mid_ref, g_out_ref):
        rows = ref.shape[0]
        for b in range(ref.shape[1] // 128):
            part = total_ref[at // half_rows, pl.ds(at % half_rows // each, rows // each)]
            ref[:, b * 128 : (b + 1) * 128] = part.reshape(rows, 128)
            at += rows


def whole_step_call(spec_in, cotangent, legendre, quad, waves_all, gain, w_in, b_in, w_mid, b_mid, w_out, n_lat, n_lev):
    slots, _, members, lanes = spec_in.shape
    kinds, n, two = 2, n_lat * n_lev, NLAT // (n_lat * n_lev)
    bf16, f32 = jnp.bfloat16, jnp.float32
    waves, longitudes = 2 * waves_all.shape[0], NLON
    params = (quad[None], spec_in, cotangent, legendre, waves_all[None], gain[None], w_in, b_in[None], w_mid, b_mid[None], w_out)
    chips = n // 2
    grad_rows = (w_in.size + w_mid.size + w_out.size) // lanes
    half = grad_rows // 2
    slices = (chips, half // chips, lanes)
    few = 8
    small = (2 * few, lanes)
    dma = pltpu.SemaphoreType.DMA
    row = lambda a: jax.ShapeDtypeStruct((1, a.size), f32)
    out_shape = (
        jax.ShapeDtypeStruct((members, slots, n, two, lanes), bf16),
        jax.ShapeDtypeStruct(w_in.shape, bf16),
        jax.ShapeDtypeStruct(w_mid.shape, bf16),
        jax.ShapeDtypeStruct(w_out.shape, bf16),
        row(gain),
        row(b_in),
        row(b_mid),
    )
    return pl.pallas_call(
        functools.partial(whole_step, n),
        out_shape=out_shape,
        in_specs=[pl.BlockSpec(memory_space=pltpu.SMEM)]
        + [pl.BlockSpec(memory_space=pltpu.VMEM)] * len(params),
        out_specs=[pl.BlockSpec(memory_space=pl.ANY)]
        + [pl.BlockSpec(memory_space=pltpu.VMEM)] * (len(out_shape) - 1),
        scratch_shapes=[
            pltpu.VMEM((members, kinds, slots, n, two, lanes), bf16),
            pltpu.VMEM((members, kinds, n_lev, n_lat * slots, two, lanes), bf16),
            pltpu.VMEM((members, n_lev, n_lat * slots, two, lanes), bf16),
            pltpu.VMEM((2 * longitudes, 2 * waves), bf16),
            pltpu.VMEM((2 * waves, 2 * longitudes), bf16),
            pltpu.VMEM((grad_rows, lanes), f32),
            pltpu.VMEM(small, f32),
            pltpu.VMEM((half, lanes), f32),
            pltpu.VMEM((few, lanes), f32),
            pltpu.VMEM(slices, bf16),
            pltpu.VMEM(slices, bf16),
            pltpu.VMEM(slices[1:], bf16),
            pltpu.VMEM((2,) + slices, bf16),
            pltpu.VMEM((few, lanes), bf16),
            pltpu.VMEM((chips, few, lanes), bf16),
            pltpu.VMEM((2, few, lanes), f32),
            dma((1,)),
            dma((members,)),
        ]
        + [dma((2,))] * 8
        + [dma((1,))],
        compiler_params=pltpu.CompilerParams(
            collective_id=0, has_side_effects=True, vmem_limit_bytes=60 * 1024 * 1024
        ),
        name="whole_step",
    )(waves_all, *params)


def local(
    n_lat, n_lev, spec_in, cotangent, legendre, quad_weights, wave_order, norm_gain, weight_in,
    bias_in, weight_mid, bias_mid, weight_out,
):
    bf16 = jnp.bfloat16
    n = n_lat * n_lev
    slots_here, degrees, members, lanes = spec_in.shape
    rows = NLAT // n
    own_waves = lax.dynamic_slice_in_dim(wave_order, lax.axis_index("lat") * slots_here, slots_here)
    living, shrink = spectral_masks(own_waves, degrees)
    basis_rows = jnp.where(living[:, :, None], legendre, jnp.zeros_like(legendre))
    lane = np.arange(lanes)
    apart = np.zeros((lanes, lanes), np.float32)
    apart[lane, (lane % 2) * (lanes // 2) + lane // 2] = 1.0
    apart = jnp.asarray(apart, bf16)

    landed, g_in, g_mid, g_out, g_gain, g_b_in, g_b_mid = whole_step_call(
        spec_in, cotangent, legendre, quad_weights, wave_order, norm_gain, weight_in, bias_in, weight_mid, bias_mid, weight_out,
        n_lat, n_lev,
    )
    landed = landed.reshape(members, slots_here, n * rows, lanes)
    landed = jnp.einsum(
        "estq,kq->setk", landed, apart, preferred_element_type=jnp.float32
    ).astype(bf16)
    grad_spec = cotangent.astype(jnp.float32) * shrink[:, :, None, None] + jnp.einsum(
        "slt,setk->slek", basis_rows, landed, preferred_element_type=jnp.float32
    )
    factor = float(MEMBERS * NLAT * NLON) ** (-0.5)
    g_in, g_mid, g_out = (g.astype(jnp.float32) * factor for g in (g_in, g_mid, g_out))
    return (grad_spec, g_gain[0], g_in, g_b_in[0], g_mid, g_b_mid[0], g_out)


def solution(mesh):
    split = P("lat", None, None, "lev")
    placed = (split, split, P("lat", None, None)) + (P(),) * 8
    return jax.shard_map(
        functools.partial(local, mesh.shape["lat"], mesh.shape["lev"]),
        mesh=mesh,
        in_specs=placed,
        out_specs=(split,) + (P(),) * 6,
        check_vma=False,
    )
```
